512 devices in a mesh: ifg: 16 (over x, y), pix: 32 (over z, core).
Axes of the slice: x: 4, y: 4, z: 16, core: 2. Of those that a mesh axis runs over, the one named last changes fastest.
Arguments:
- phase: bfloat16 [1200, 49152], P('ifg', 'pix'), may hold values from -8 to 8
- incidence: int32 [2304, 1200], P('ifg'), may hold values from -1 to 1, as said below
- triplet_weight: float32 [2304], P('ifg'), may hold values from 0.3 to 3
- date_pairs: int32 [1200, 2], P('ifg'), may hold values from 0 to 249, as said below
Outputs:
- residual: float32 [2304, 49152], P('ifg', 'pix')
- relative: float32 [49152], P('pix')
- corrected: float32 [1200, 49152], P('ifg', 'pix')
The draws below stay inside these ranges and needn't reach their ends.
Inputs may be any that keep to these rules, and one draw needn't show every extreme that they name: `incidence`: each row is a closure triplet of three dates a < b < c whose three interferograms all appear in date_pairs: +1 on (a, b) and on (b, c), -1 on (a, c), zeros elsewhere. No two rows are equal. `date_pairs`: interferograms are listed by first date, then by second date; the second date is 1 to 5 dates after the first, and no pair appears twice.
All inputs are finite; a program needn't handle non-finite values.
Results may differ from the reference program's by a relative error of at most 0.013.
Values may be sent and summed in bfloat16 or wider, within the bound.
A program may use at most 64 MiB of HBM per device.

```python
import math
import jax
import jax.numpy as jnp
import numpy as np
from jax import lax

TRIPLETS = 2304
IFGS = 1200
DATES = 250
P_DEV = 1536
PIXELS = 49152
N_IFG = 16


def network(key):
    extra = IFGS - (4 * DATES - 10)
    starts = lax.broadcasted_iota(jnp.int32, (DATES, 5), 0)
    spans = lax.broadcasted_iota(jnp.int32, (DATES, 5), 1) + 1
    candidates = DATES - 5
    longer = jax.random.randint(jax.random.fold_in(key, 21), (candidates,), 0, 1 << 16, dtype=jnp.int32)
    longer = longer * candidates + lax.broadcasted_iota(jnp.int32, (candidates,), 0)
    _, picked = lax.top_k(longer, extra)
    marks = jnp.sum((lax.broadcasted_iota(jnp.int32, (DATES, extra), 0) == picked[None, :]).astype(jnp.int32), axis=1)
    inside = (starts + spans <= DATES - 1).astype(jnp.int32)
    exists = jnp.where(spans <= 4, inside, marks[:, None] * inside).astype(jnp.int32)
    flat = exists.reshape(-1)
    places = lax.broadcasted_iota(jnp.int32, (DATES * 5,), 0)
    order = jnp.argsort(jnp.where(flat == 1, places, (1 << 20) + places), stable=True)[:IFGS].astype(jnp.int32)
    first = order // 5
    second = first + order % 5 + 1
    pairs = jnp.stack([first, second], axis=1).astype(jnp.int32)
    rank = (jnp.cumsum(flat) - 1).astype(jnp.int32).reshape(DATES, 5)
    combos = [(p, q) for p in range(1, 5) for q in range(1, 5) if p + q <= 5]
    left = jnp.array(np.array([c[0] for c in combos], dtype=np.int32))
    right = jnp.array(np.array([c[1] for c in combos], dtype=np.int32))
    count = len(combos)
    anchor = lax.broadcasted_iota(jnp.int32, (DATES, count), 0)
    short_a = jnp.broadcast_to(left[None, :], (DATES, count))
    short_b = jnp.broadcast_to(right[None, :], (DATES, count))
    middle = jnp.minimum(anchor + short_a, DATES - 1)
    valid = exists[anchor, short_a - 1] * exists[middle, short_b - 1] * exists[anchor, short_a + short_b - 1]
    total = DATES * count
    noise = jax.random.randint(jax.random.fold_in(key, 22), (total,), 0, 1 << 10, dtype=jnp.int32)
    scores = valid.reshape(-1) * (1 << 24) + noise * total + lax.broadcasted_iota(jnp.int32, (total,), 0)
    _, chosen = lax.top_k(scores, TRIPLETS)
    chosen = chosen.astype(jnp.int32)
    row_a = chosen // count
    which = chosen % count
    span_a = left[which]
    span_b = right[which]
    row_mid = jnp.minimum(row_a + span_a, DATES - 1)
    col_one = rank[row_a, span_a - 1]
    col_two = rank[row_mid, span_b - 1]
    col_long = rank[row_a, span_a + span_b - 1]
    columns = lax.broadcasted_iota(jnp.int32, (TRIPLETS, IFGS), 1)
    signed = (columns == col_one[:, None]).astype(jnp.int32) + (columns == col_two[:, None]).astype(jnp.int32) - (columns == col_long[:, None]).astype(jnp.int32)
    return (signed.astype(jnp.int32), pairs)


def draw_incidence(key, part):
    signed, _ = network(jax.random.fold_in(key, 5))
    return signed


def draw_date_pairs(key, part):
    _, pairs = network(jax.random.fold_in(key, 5))
    return pairs


def draw_phase(key, part):
    block_width = max(P_DEV // 2, 1)
    block_count = PIXELS // block_width
    block_of = (lax.broadcasted_iota(jnp.int32, (PIXELS,), 0) // block_width).astype(jnp.int32)
    inner = jax.random.fold_in(key, 31)
    level_key = jax.random.fold_in(key, 32)
    overall_key = jax.random.fold_in(key, 33)
    rough_key = jax.random.fold_in(key, 34)
    rough = jax.random.uniform(rough_key, (1, PIXELS), jnp.float32, 0.7, 1.4)
    levels = jax.random.uniform(level_key, (block_count,), jnp.float32, -1.0, 0.6)
    overall = 0.25 * jnp.exp(jax.random.uniform(overall_key, (), jnp.float32, -0.5, 0.5))
    spread = overall * jnp.power(10.0, jnp.take(levels, block_of))[None, :] * rough
    values = jnp.clip(jax.random.normal(inner, (IFGS, PIXELS), jnp.float32), -3.0, 3.0) * spread
    return values.astype(jnp.bfloat16)


def shard_levels(own_key, dims, shards, least, top_value):
    def one(dim, blocks):
        steps = jax.random.uniform(jax.random.fold_in(jax.random.fold_in(own_key, 6), dim), (blocks,), jnp.float32, least / len(shards), top_value / len(shards))
        return jnp.repeat(jnp.exp(steps), dims[dim] // blocks).reshape((-1,) + (1,) * (len(dims) - dim - 1))

    level = one(*shards[0])
    for cut in shards[1:]:
        level = level * one(*cut)
    return level


def setup_inputs(seed: int = 0) -> dict:
    seeds = jax.random.split(jax.random.key(seed), 5)
    return {
        "phase": draw_phase(jax.random.fold_in(seeds[4], 71), 0),
        "incidence": draw_incidence(jax.random.fold_in(seeds[4], 71), 0),
        "triplet_weight": jnp.clip(jnp.exp(math.log(3.0) - 2.3025851 * jax.random.uniform(seeds[2], (TRIPLETS,), jnp.float32) ** shard_levels(seeds[2], (TRIPLETS,), ((0, 16),), -0.2, 0.2)), 0.3, 3.0),
        "date_pairs": draw_date_pairs(jax.random.fold_in(seeds[4], 71), 0),
    }


def reference(phase, incidence, triplet_weight, date_pairs):
    signed = incidence.astype(jnp.bfloat16)
    closure = jnp.dot(signed, phase, preferred_element_type=jnp.float32)
    residual = jnp.sin(closure)
    wrapped = residual.astype(jnp.bfloat16)
    misfit = jnp.sum(triplet_weight[:, None] * (1.0 - jnp.cos(closure)), axis=0)
    score = misfit / jnp.sum(triplet_weight)
    relative = score / (jnp.sum(score) / PIXELS)
    blocks = N_IFG
    rows = TRIPLETS // blocks
    signed_blocks = signed.reshape(blocks, rows, IFGS)
    wrapped_blocks = wrapped.reshape(blocks, rows, PIXELS)

    def accumulate(carry, pair):
        part = lax.dot_general(pair[0], pair[1], (((0,), (0,)), ((), ())), preferred_element_type=jnp.float32)
        return carry + part.astype(jnp.bfloat16).astype(jnp.float32), None

    correction, _ = lax.scan(accumulate, jnp.zeros((IFGS, PIXELS), jnp.float32), (signed_blocks, wrapped_blocks))
    span = (date_pairs[:, 1] - date_pairs[:, 0]).astype(jnp.float32)
    corrected = phase.astype(jnp.float32) - correction / (2.0 + span)[:, None]
    return residual, relative, corrected
```

```python
import jax
import jax.numpy as jnp
from jax import lax
from jax.experimental import pallas as pl
from jax.experimental.pallas import tpu as pltpu
from jax.sharding import PartitionSpec as P

GROUP = 16
LANES = 128
INV_PI = 0.3183098861837907
PI_HI = 3.140625
PI_LO = 9.676535897932e-4
SIN = (-0.16666657096162138, 0.008333017284575896, -0.00019806614761156636, 2.6000538932920348e-06)
COS = (0.4999999954954239, -0.04166664072751474, 0.0013888403501702445, -2.476188593339371e-05, 2.607710003258223e-07)


def poly(coefs, z):
    out = jnp.full_like(z, coefs[-1])
    for c in coefs[-2::-1]:
        out = out * z + c
    return out


def sin_and_loss(x):
    k = jnp.floor(x * INV_PI + 0.5)
    r = (x - k * PI_HI) - k * PI_LO
    half = k * 0.5
    odd2 = (half - jnp.floor(half)) * 4.0
    sign = 1.0 - odd2
    z = r * r
    sine = sign * (r + (r * z) * poly(SIN, z))
    loss = odd2 + sign * (z * poly(COS, z))
    return sine, loss


def rank_of(device, core):
    return lax.rem(lax.rem(device, 4) - device // 4 - 2 * core + 7, 4)


def kernel(
    phase_ref, idx_ref, res_ref, cor_ref, score_ref,
    padded, ph, pht, idxs, tiles, inct, iota, wb, cb, acc, row,
    idx_s, idx_r, ph_s, ph_r, res_s, res_r, lef_s, lef_r, cor_s, cor_r, sc_s, sc_r,
):
    me = lax.axis_index("ifg")
    core = lax.rem(lax.axis_index("pix"), 2)
    rank = rank_of(me, core)
    active = rank < 3
    share = 3 * (me // 4) + rank
    my_lanes = pl.ds(pl.multiple_of(share * LANES, LANES), LANES)
    rows = phase_ref.shape[0]
    depth = padded.shape[0]

    barrier = pltpu.get_barrier_semaphore()

    @pl.loop(1, GROUP)
    def _(k):
        pl.semaphore_signal(barrier, inc=1, device_id={"ifg": lax.rem(me + k, GROUP)}, device_id_type=pl.DeviceIdType.MESH)

    padded[...] = jnp.zeros_like(padded)
    padded[0:rows, :] = phase_ref[...]
    iota[...] = lax.broadcasted_iota(jnp.int32, iota.shape, 0).astype(jnp.float32).astype(jnp.bfloat16)
    acc[...] = jnp.zeros_like(acc)

    pl.semaphore_wait(barrier, GROUP - 1)

    def put(src, dst, send, recv, device):
        @pl.when(device != me)
        def _():
            pltpu.make_async_remote_copy(
                src_ref=src, dst_ref=dst, send_sem=send, recv_sem=recv,
                device_id={"ifg": device}, device_id_type=pl.DeviceIdType.MESH,
            ).start()

        @pl.when(device == me)
        def _():
            pltpu.make_async_copy(src, dst, recv).start()

    def took(ref, sem):
        pltpu.make_async_copy(ref, ref, sem).wait()

    def to_shares(body):
        @pl.loop(0, GROUP)
        def _(k):
            device = lax.rem(me + k, GROUP)
            their = rank_of(device, core)

            @pl.when(their < 3)
            def _():
                body(device, pl.multiple_of((3 * (device // 4) + their) * LANES, LANES))

    to_shares(lambda d, at: put(idx_ref, idxs.at[me], idx_s.at[d], idx_r.at[me], d))
    to_shares(lambda d, at: put(padded.at[:, pl.ds(at, LANES)], ph.at[me], ph_s.at[d], ph_r.at[me], d))

    @pl.when(active)
    def _():
        @pl.loop(0, GROUP)
        def _(d):
            took(idxs.at[d], idx_r.at[d])

        for p in range(GROUP // 2):
            tiles[p, :, 0:LANES] = idxs[2 * p, :, 0:LANES]
            tiles[p, :, LANES:] = idxs[2 * p + 1, :, 0:LANES]
        for q in range(2):
            rest = idxs[8 * q, :, LANES:]
            for i in range(1, 8):
                rest = rest + idxs[8 * q + i, :, LANES:]
            tiles[GROUP // 2, :, q * LANES : (q + 1) * LANES] = rest

        @pl.loop(0, GROUP // 2 + 1)
        def _(p):
            t = tiles[p]

            @pl.loop(0, GROUP)
            def _(b):
                rel = (t - lax.convert_element_type(b * depth, jnp.float32)).astype(jnp.bfloat16)
                at = iota[...]
                one = jnp.ones(at.shape, jnp.bfloat16)
                both = jnp.logical_or(at == rel[0:1], at == rel[1:2])
                signed = jnp.where(at == rel[2:3], -one, jnp.where(both, one, jnp.zeros_like(one)))
                inct[p, pl.ds(pl.multiple_of(b * depth, depth), depth), :] = signed

        for half in range(2):
            for d in range(8 * half, 8 * half + 8):
                took(ph.at[d], ph_r.at[d])
            block = ph[8 * half : 8 * half + 8].reshape(8 * depth, LANES)
            pht[:, 8 * depth * half : 8 * depth * (half + 1)] = jnp.transpose(block.astype(jnp.float32)).astype(jnp.bfloat16)

        def closures(p):
            closure = jnp.dot(pht[...], inct[p], preferred_element_type=jnp.float32)
            sine, loss = sin_and_loss(closure)
            acc[...] += loss * tiles[p, 3:4, :]
            wb[p] = jnp.transpose(sine).astype(jnp.bfloat16)

        @pl.loop(0, GROUP // 2)
        def _(j):
            p = lax.rem(me // 2 + j, GROUP // 2)
            closures(p)
            for q in range(2):
                d = 2 * p + q
                put(wb.at[p, pl.ds(q * LANES, LANES)], res_ref.at[pl.ds(0, LANES), my_lanes], res_s.at[d], res_r.at[share], d)

        closures(GROUP // 2)

        @pl.loop(0, GROUP)
        def _(k):
            d = lax.rem(me + k, GROUP)
            put(
                wb.at[GROUP // 2, pl.ds(pl.multiple_of(16 * d, 16), 16)],
                res_ref.at[pl.ds(LANES, 16), my_lanes], lef_s.at[d], lef_r.at[share], d,
            )

        total = tiles[0, 3:4, :]
        for p in range(1, GROUP // 2 + 1):
            total = total + tiles[p, 3:4, :]
        both = acc[:, 0:LANES] + acc[:, LANES:]
        misfit = jnp.sum(jnp.transpose(both), axis=0, keepdims=True)
        row[...] = misfit / jnp.sum(total, axis=1, keepdims=True)

        @pl.loop(0, 4)
        def _(j):
            c = lax.rem(me // 4 + j, 4)
            at = pl.ds(pl.multiple_of(c * 4 * depth, 4 * depth), 4 * depth)
            corr = jnp.zeros((4 * depth, LANES), jnp.float32)
            for p in range(GROUP // 2 + 1):
                corr = corr + jnp.dot(inct[p, at, :], wb[p], preferred_element_type=jnp.float32)
            cb[pl.ds(4 * c, 4)] = corr.astype(jnp.bfloat16).reshape(4, depth, LANES)
            for q in range(4):
                d = 4 * c + q
                put(cb.at[d], cor_ref.at[:, my_lanes], cor_s.at[d], cor_r.at[share], d)

        @pl.loop(0, GROUP)
        def _(k):
            d = lax.rem(me + k, GROUP)
            put(row, score_ref.at[share], sc_s.at[d], sc_r.at[share], d)

    @pl.loop(0, 12)
    def _(s):
        lanes = pl.ds(pl.multiple_of(s * LANES, LANES), LANES)
        took(res_ref.at[pl.ds(0, LANES), lanes], res_r.at[s])
        took(res_ref.at[pl.ds(LANES, 16), lanes], lef_r.at[s])
        took(cor_ref.at[:, lanes], cor_r.at[s])
        took(score_ref.at[s], sc_r.at[s])

    @pl.loop(1, GROUP)
    def _(k):
        d = lax.rem(me + k, GROUP)

        @pl.when(rank_of(d, core) < 3)
        def _():
            took(idxs.at[0], idx_s.at[d])
            took(ph.at[0], ph_s.at[d])

        @pl.when(active)
        def _():
            took(wb.at[0, pl.ds(0, LANES)], res_s.at[d])
            took(wb.at[0, pl.ds(0, 16)], lef_s.at[d])
            took(cb.at[0], cor_s.at[d])
            took(row, sc_s.at[d])


def local(phase, incidence, triplet_weight, date_pairs):
    rows, pixel_count = phase.shape
    depth = -(-rows // 16) * 16
    triplets, width = incidence.shape
    me = lax.axis_index("ifg")
    columns = lax.broadcasted_iota(jnp.int32, incidence.shape, 1)
    columns = (columns + (columns // rows) * (depth - rows)).astype(jnp.float32)
    plus = incidence == 1
    first = jnp.min(jnp.where(plus, columns, 4096.0), axis=1)
    second = jnp.max(jnp.where(plus, columns, -1.0), axis=1)
    long = jnp.sum(jnp.where(incidence == -1, columns, 0.0), axis=1)
    four = jnp.stack([first, second, long, triplet_weight])
    lane = lax.broadcasted_iota(jnp.int32, (4, LANES), 1)
    rest = jnp.where(lane // 16 == lax.rem(me, 8), jnp.tile(four[:, LANES:], (1, 8)), 0.0)
    idx = jnp.pad(jnp.concatenate([four[:, :LANES], rest], axis=1), ((0, 4), (0, 0)))

    shares = pixel_count // LANES
    pairs = GROUP // 2 + 1
    vmem = pl.BlockSpec(memory_space=pltpu.VMEM)
    sems = [pltpu.SemaphoreType.DMA((GROUP,))] * 12
    residual, correction, score = pl.pallas_call(
        kernel,
        out_shape=(
            jax.ShapeDtypeStruct((triplets, pixel_count), jnp.bfloat16),
            jax.ShapeDtypeStruct((depth, pixel_count), jnp.bfloat16),
            jax.ShapeDtypeStruct((shares, 1, LANES), jnp.float32),
        ),
        in_specs=[vmem] * 2,
        out_specs=[vmem] * 3,
        scratch_shapes=[
            pltpu.VMEM((depth, pixel_count), jnp.bfloat16),
            pltpu.VMEM((GROUP, depth, LANES), jnp.bfloat16),
            pltpu.VMEM((LANES, GROUP * depth), jnp.bfloat16),
            pltpu.VMEM((GROUP, 8, 2 * LANES), jnp.float32),
            pltpu.VMEM((pairs, 8, 2 * LANES), jnp.float32),
            pltpu.VMEM((pairs, GROUP * depth, 2 * LANES), jnp.bfloat16),
            pltpu.VMEM((depth, 2 * LANES), jnp.bfloat16),
            pltpu.VMEM((pairs, 2 * LANES, LANES), jnp.bfloat16),
            pltpu.VMEM((GROUP, depth, LANES), jnp.bfloat16),
            pltpu.VMEM((LANES, 2 * LANES), jnp.float32),
            pltpu.VMEM((1, LANES), jnp.float32),
            *sems,
        ],
        compiler_params=pltpu.CompilerParams(collective_id=0, has_side_effects=True),
    )(phase, idx)

    score = score.reshape(pixel_count)
    all_pixels = pixel_count * lax.axis_size("pix")
    relative = score / (lax.psum(jnp.sum(score), "pix") / all_pixels)
    span = (date_pairs[:, 1] - date_pairs[:, 0]).astype(jnp.float32)
    corrected = phase.astype(jnp.float32) - correction[:rows].astype(jnp.float32) / (2.0 + span)[:, None]
    return (residual.astype(jnp.float32), relative, corrected)


def solution(mesh):
    return jax.shard_map(
        local,
        mesh=mesh,
        in_specs=(P("ifg", "pix"), P("ifg", None), P("ifg"), P("ifg", None)),
        out_specs=(P("ifg", "pix"), P("pix"), P("ifg", "pix")),
        check_vma=False,
    )
```

```python
import functools

import jax
import jax.numpy as jnp
from jax import lax
from jax.experimental import pallas as pl
from jax.experimental.pallas import tpu as pltpu
from jax.sharding import PartitionSpec as P

GROUP = 16
LANES = 128
INV_PI = 0.3183098861837907
PI_HI = 3.140625
PI_LO = 9.676535897932e-4
SIN = (-0.16666657096162138, 0.008333017284575896, -0.00019806614761156636, 2.6000538932920348e-06)
COS = (0.4999999954954239, -0.04166664072751474, 0.0013888403501702445, -2.476188593339371e-05, 2.607710003258223e-07)


def poly(coefs, z):
    out = jnp.full_like(z, coefs[-1])
    for c in coefs[-2::-1]:
        out = out * z + c
    return out


def sin_and_loss(x):
    k = jnp.floor(x * INV_PI + 0.5)
    r = (x - k * PI_HI) - k * PI_LO
    half = k * 0.5
    odd2 = (half - jnp.floor(half)) * 4.0
    sign = 1.0 - odd2
    z = r * r
    sine = sign * (r + (r * z) * poly(SIN, z))
    loss = odd2 + sign * (z * poly(COS, z))
    return sine, loss


def rank_of(device, core):
    return lax.rem(lax.rem(device, 4) - device // 4 - 2 * core + 7, 4)


def kernel(
    all_pixels,
    phase_ref, inc_hbm, weight_ref, res_ref, cor_ref, rel_ref,
    inc, idx, rest16, wrow, padded, ph, pht, idxs, tiles, inct, iota, wb, cb, acc, scores, fin_out, fin,
    inc_sem, idx_s, idx_r, ph_s, ph_r, res_s, res_r, lef_s, lef_r, cor_s, cor_r, fin_s, fin_r, pix_s, pix_r,
    near1, near2, near4,
):
    me = lax.axis_index("ifg")
    pix = lax.axis_index("pix")
    core = lax.rem(pix, 2)
    rank = rank_of(me, core)
    active = rank < 3
    share = 3 * (me // 4) + rank
    my_lanes = pl.ds(pl.multiple_of(share * LANES, LANES), LANES)
    rows = phase_ref.shape[0]
    depth = padded.shape[0]

    pixes = scores.shape[0]

    barrier = pltpu.get_barrier_semaphore()

    def tell_group(k):
        pl.semaphore_signal(barrier, inc=1, device_id={"ifg": lax.rem(me + k, GROUP)}, device_id_type=pl.DeviceIdType.MESH)

    def tell_pix(sem, other):
        pl.semaphore_signal(sem, inc=1, device_id={"pix": lax.rem(other, pixes)}, device_id_type=pl.DeviceIdType.MESH)

    def tell_along_z(sem, distance):
        tell_pix(sem, pix + 2 * distance)
        tell_pix(sem, pix + pixes - 2 * distance)

    pl.loop(1, GROUP)(tell_group)
    across = 2 * (pix // 2) + 1 - core
    tell_pix(barrier, across)
    tell_along_z(barrier, 1)
    tell_pix(barrier, across + 2)
    tell_pix(barrier, across + pixes - 2)
    read_inc = pltpu.make_async_copy(inc_hbm, inc, inc_sem)
    read_inc.start()

    padded[...] = jnp.zeros_like(padded)
    padded[0:rows, :] = phase_ref[...]
    iota[...] = lax.broadcasted_iota(jnp.int32, iota.shape, 0).astype(jnp.float32).astype(jnp.bfloat16)
    acc[...] = jnp.zeros_like(acc)

    scores[pix] = jnp.zeros(scores.shape[1:], scores.dtype)
    fin_out[...] = jnp.zeros_like(fin_out)
    wrow[...] = jnp.zeros_like(wrow)
    wrow[0:1, 0 : weight_ref.shape[1]] = weight_ref[...]
    rest16[...] = jnp.zeros_like(rest16)

    read_inc.wait()
    width = inc.shape[1]
    column = lax.broadcasted_iota(jnp.int32, (1, width), 1).astype(jnp.float32)
    column = column + jnp.floor((column + 0.5) * (1.0 / rows)) * (depth - rows)
    value = inc[...]
    plus = value == 1
    first = jnp.min(jnp.where(plus, column, 4096.0), axis=1, keepdims=True)
    second = jnp.max(jnp.where(plus, column, -1.0), axis=1, keepdims=True)
    long = jnp.sum(jnp.where(value == -1, column, 0.0), axis=1, keepdims=True)
    lane = lax.broadcasted_iota(jnp.int32, (inc.shape[0], LANES), 1)
    three = jnp.where(lane == 0, first, jnp.where(lane == 1, second, long))
    spot = 16 * lax.rem(me, 8)
    rest16[pl.ds(pl.multiple_of(spot, 16), 16), :] = three[LANES:]
    line = lax.broadcasted_iota(jnp.int32, (8, LANES), 0)
    for q, t, w in (
        (0, three[:LANES], wrow[:, :LANES]),
        (1, rest16[...], pltpu.roll(wrow[:, LANES:], spot, 1)),
    ):
        t = jnp.where(line < 3, jnp.transpose(t)[0:8], 0.0)
        idx[:, q * LANES : (q + 1) * LANES] = jnp.where(line == 3, jnp.broadcast_to(w[0:1], t.shape), t)

    pl.semaphore_wait(barrier, GROUP + 4)
    tell_along_z(near1, 1)

    def put(src, dst, send, recv, device):
        @pl.when(device != me)
        def _():
            pltpu.make_async_remote_copy(
                src_ref=src, dst_ref=dst, send_sem=send, recv_sem=recv,
                device_id={"ifg": device}, device_id_type=pl.DeviceIdType.MESH,
            ).start()

        @pl.when(device == me)
        def _():
            pltpu.make_async_copy(src, dst, recv).start()

    def took(ref, sem):
        pltpu.make_async_copy(ref, ref, sem).wait()

    def to_shares(body):
        @pl.loop(0, GROUP)
        def _(k):
            device = lax.rem(me + k, GROUP)
            their = rank_of(device, core)

            @pl.when(their < 3)
            def _():
                body(device, pl.multiple_of((3 * (device // 4) + their) * LANES, LANES))

    to_shares(lambda d, at: put(idx, idxs.at[me], idx_s.at[d], idx_r.at[me], d))
    to_shares(lambda d, at: put(padded.at[:, pl.ds(at, LANES)], ph.at[me], ph_s.at[d], ph_r.at[me], d))

    @pl.when(active)
    def _():
        @pl.loop(0, GROUP)
        def _(d):
            took(idxs.at[d], idx_r.at[d])

        for p in range(GROUP // 2):
            tiles[p, :, 0:LANES] = idxs[2 * p, :, 0:LANES]
            tiles[p, :, LANES:] = idxs[2 * p + 1, :, 0:LANES]
        for q in range(2):
            rest = idxs[8 * q, :, LANES:]
            for i in range(1, 8):
                rest = rest + idxs[8 * q + i, :, LANES:]
            tiles[GROUP // 2, :, q * LANES : (q + 1) * LANES] = rest

        @pl.loop(0, GROUP // 2 + 1)
        def _(p):
            t = tiles[p]

            @pl.loop(0, GROUP)
            def _(b):
                rel = (t - lax.convert_element_type(b * depth, jnp.float32)).astype(jnp.bfloat16)
                at = iota[...]
                one = jnp.ones(at.shape, jnp.bfloat16)
                both = jnp.logical_or(at == rel[0:1], at == rel[1:2])
                signed = jnp.where(at == rel[2:3], -one, jnp.where(both, one, jnp.zeros_like(one)))
                inct[p, pl.ds(pl.multiple_of(b * depth, depth), depth), :] = signed

    pl.semaphore_wait(near1, 2)
    tell_along_z(near2, 2)

    @pl.when(active)
    def _():
        for half in range(2):
            for d in range(8 * half, 8 * half + 8):
                took(ph.at[d], ph_r.at[d])
            block = ph[8 * half : 8 * half + 8].reshape(8 * depth, LANES)
            pht[:, 8 * depth * half : 8 * depth * (half + 1)] = jnp.transpose(block.astype(jnp.float32)).astype(jnp.bfloat16)

    pl.semaphore_wait(near2, 2)
    tell_along_z(near4, 4)

    @pl.when(active)
    def _():
        def closures(p):
            closure = jnp.dot(pht[...], inct[p], preferred_element_type=jnp.float32)
            sine, loss = sin_and_loss(closure)
            acc[...] += loss * tiles[p, 3:4, :]
            wb[p] = jnp.transpose(sine).astype(jnp.bfloat16)

        @pl.loop(0, GROUP // 2)
        def _(j):
            p = lax.rem(me // 2 + j, GROUP // 2)
            closures(p)
            for q in range(2):
                d = 2 * p + q
                put(wb.at[p, pl.ds(q * LANES, LANES)], res_ref.at[pl.ds(0, LANES), my_lanes], res_s.at[d], res_r.at[share], d)

        closures(GROUP // 2)

        @pl.loop(0, GROUP)
        def _(k):
            d = lax.rem(me + k, GROUP)
            put(
                wb.at[GROUP // 2, pl.ds(pl.multiple_of(16 * d, 16), 16)],
                res_ref.at[pl.ds(LANES, 16), my_lanes], lef_s.at[d], lef_r.at[share], d,
            )

        total = tiles[0, 3:4, :]
        for p in range(1, GROUP // 2 + 1):
            total = total + tiles[p, 3:4, :]
        both = acc[:, 0:LANES] + acc[:, LANES:]
        misfit = jnp.sum(jnp.transpose(both), axis=0, keepdims=True)
        scores[pix] = misfit / jnp.sum(total, axis=1, keepdims=True)

    pl.semaphore_wait(near4, 2)

    @pl.loop(1, pixes)
    def _(k):
        other = lax.rem(pix + k, pixes)
        pltpu.make_async_remote_copy(
            src_ref=scores.at[pix], dst_ref=scores.at[pix], send_sem=pix_s.at[other], recv_sem=pix_r.at[pix],
            device_id={"pix": other}, device_id_type=pl.DeviceIdType.MESH,
        ).start()

    @pl.when(active)
    def _():
        @pl.loop(0, 4)
        def _(j):
            c = lax.rem(me // 4 + j, 4)
            at = pl.ds(pl.multiple_of(c * 4 * depth, 4 * depth), 4 * depth)
            corr = jnp.zeros((4 * depth, LANES), jnp.float32)
            for p in range(GROUP // 2 + 1):
                corr = corr + jnp.dot(inct[p, at, :], wb[p], preferred_element_type=jnp.float32)
            cb[pl.ds(4 * c, 4)] = corr.astype(jnp.bfloat16).reshape(4, depth, LANES)
            for q in range(4):
                d = 4 * c + q
                put(cb.at[d], cor_ref.at[:, my_lanes], cor_s.at[d], cor_r.at[share], d)

    @pl.loop(1, pixes)
    def _(k):
        other = lax.rem(pix + k, pixes)
        took(scores.at[other], pix_r.at[other])

    fin_out[0:1] = scores[pix]
    fin_out[1:2] = jnp.sum(scores[...], axis=0)
    slot = jnp.where(active, share, 12 + me // 4)

    @pl.loop(0, GROUP)
    def _(k):
        d = lax.rem(me + k, GROUP)
        put(fin_out, fin.at[slot], fin_s.at[d], fin_r.at[slot], d)

    @pl.loop(0, 12)
    def _(s):
        lanes = pl.ds(pl.multiple_of(s * LANES, LANES), LANES)
        took(res_ref.at[pl.ds(0, LANES), lanes], res_r.at[s])
        took(res_ref.at[pl.ds(LANES, 16), lanes], lef_r.at[s])
        took(cor_ref.at[:, lanes], cor_r.at[s])

    @pl.loop(0, GROUP)
    def _(s):
        took(fin.at[s], fin_r.at[s])

    everything = jnp.sum(jnp.sum(fin[...], axis=0)[1:2], axis=1, keepdims=True)
    for s in range(12):
        rel_ref[s] = fin[s, 0:1] / (everything / all_pixels)

    @pl.loop(1, pixes)
    def _(k):
        other = lax.rem(pix + k, pixes)
        took(scores.at[pix], pix_s.at[other])

    @pl.loop(1, GROUP)
    def _(k):
        d = lax.rem(me + k, GROUP)

        took(fin_out, fin_s.at[d])

        @pl.when(rank_of(d, core) < 3)
        def _():
            took(idxs.at[0], idx_s.at[d])
            took(ph.at[0], ph_s.at[d])

        @pl.when(active)
        def _():
            took(wb.at[0, pl.ds(0, LANES)], res_s.at[d])
            took(wb.at[0, pl.ds(0, 16)], lef_s.at[d])
            took(cb.at[0], cor_s.at[d])


def local(phase, incidence, triplet_weight, date_pairs):
    rows, pixel_count = phase.shape
    depth = -(-rows // 16) * 16
    triplets = incidence.shape[0]
    shares = pixel_count // LANES
    pairs = GROUP // 2 + 1
    vmem = pl.BlockSpec(memory_space=pltpu.VMEM)
    pixes = lax.axis_size("pix")
    sems = [pltpu.SemaphoreType.DMA((GROUP,))] * 12
    residual, correction, relative = pl.pallas_call(
        functools.partial(kernel, pixes * pixel_count),
        out_shape=(
            jax.ShapeDtypeStruct((triplets, pixel_count), jnp.bfloat16),
            jax.ShapeDtypeStruct((depth, pixel_count), jnp.bfloat16),
            jax.ShapeDtypeStruct((shares, 1, LANES), jnp.float32),
        ),
        in_specs=[vmem, pl.BlockSpec(memory_space=pl.ANY), vmem],
        out_specs=[vmem] * 3,
        scratch_shapes=[
            pltpu.VMEM(incidence.shape, jnp.int32),
            pltpu.VMEM((8, 2 * LANES), jnp.float32),
            pltpu.VMEM((LANES, LANES), jnp.float32),
            pltpu.VMEM((8, 2 * LANES), jnp.float32),
            pltpu.VMEM((depth, pixel_count), jnp.bfloat16),
            pltpu.VMEM((GROUP, depth, LANES), jnp.bfloat16),
            pltpu.VMEM((LANES, GROUP * depth), jnp.bfloat16),
            pltpu.VMEM((GROUP, 8, 2 * LANES), jnp.float32),
            pltpu.VMEM((pairs, 8, 2 * LANES), jnp.float32),
            pltpu.VMEM((pairs, GROUP * depth, 2 * LANES), jnp.bfloat16),
            pltpu.VMEM((depth, 2 * LANES), jnp.bfloat16),
            pltpu.VMEM((pairs, 2 * LANES, LANES), jnp.bfloat16),
            pltpu.VMEM((GROUP, depth, LANES), jnp.bfloat16),
            pltpu.VMEM((LANES, 2 * LANES), jnp.float32),
            pltpu.VMEM((pixes, 1, LANES), jnp.float32),
            pltpu.VMEM((2, LANES), jnp.float32),
            pltpu.VMEM((GROUP, 2, LANES), jnp.float32),
            pltpu.SemaphoreType.DMA,
            *sems,
            pltpu.SemaphoreType.DMA((pixes,)),
            pltpu.SemaphoreType.DMA((pixes,)),
            pltpu.SemaphoreType.REGULAR,
            pltpu.SemaphoreType.REGULAR,
            pltpu.SemaphoreType.REGULAR,
        ],
        compiler_params=pltpu.CompilerParams(collective_id=0, has_side_effects=True),
    )(phase, incidence, triplet_weight.reshape(1, triplets))

    span = (date_pairs[:, 1] - date_pairs[:, 0]).astype(jnp.float32)
    corrected = phase.astype(jnp.float32) - correction[:rows].astype(jnp.float32) / (2.0 + span)[:, None]
    return (residual.astype(jnp.float32), relative.reshape(pixel_count), corrected)


def solution(mesh):
    return jax.shard_map(
        local,
        mesh=mesh,
        in_specs=(P("ifg", "pix"), P("ifg", None), P("ifg"), P("ifg", None)),
        out_specs=(P("ifg", "pix"), P("pix"), P("ifg", "pix")),
        check_vma=False,
    )
```

```python
import functools

import jax
import jax.numpy as jnp
from jax import lax
from jax.experimental import pallas as pl
from jax.experimental.pallas import tpu as pltpu
from jax.sharding import PartitionSpec as P

GROUP = 16
LANES = 128
VMEM = 16 * 1024 * 1024
INV_PI = 0.3183098861837907
PI_HI = 3.140625
PI_LO = 9.676535897932e-4
SIN = (-0.16666657096162138, 0.008333017284575896, -0.00019806614761156636, 2.6000538932920348e-06)
COS = (0.4999999954954239, -0.04166664072751474, 0.0013888403501702445, -2.476188593339371e-05, 2.607710003258223e-07)


def poly(coefs, z):
    out = jnp.full_like(z, coefs[-1])
    for c in coefs[-2::-1]:
        out = out * z + c
    return out


def sin_and_loss(x):
    k = jnp.floor(x * INV_PI + 0.5)
    r = (x - k * PI_HI) - k * PI_LO
    half = k * 0.5
    odd2 = (half - jnp.floor(half)) * 4.0
    sign = 1.0 - odd2
    z = r * r
    sine = sign * (r + (r * z) * poly(SIN, z))
    loss = odd2 + sign * (z * poly(COS, z))
    return sine, loss


def rank_of(device, core):
    return lax.rem(lax.rem(device, 4) - device // 4 - 2 * core + 7, 4)


def kernel(
    all_pixels,
    phase_hbm, inc_hbm, weight_hbm, dates_hbm, residual_ref, rel_ref, corrected_ref,
    inc, phase, weight, dates, res_ref, cor_ref, idx, rest16, wrow, padded, ph, pht, idxs, tiles, inct, iota, clo, wb, cb, acc, scores, fin_out, fin,
    in_sem, idx_s, idx_r, ph_s, ph_r, res_s, res_r, lef_s, lef_r, cor_s, cor_r, fin_s, fin_r, pix_s, pix_r,
    near1, near2, near4,
):
    me = lax.axis_index("ifg")
    pix = lax.axis_index("pix")
    x, y = me // 4, lax.rem(me, 4)
    core = lax.rem(pix, 2)
    rank = rank_of(me, core)
    active = rank < 3
    share = 3 * x + rank
    my_lanes = pl.ds(pl.multiple_of(share * LANES, LANES), LANES)
    rows = phase.shape[0]
    depth = padded.shape[0]
    pixes = scores.shape[0]
    steps = GROUP // 2 + 1

    def peer(j):
        return 4 * lax.rem(x + j // 4 + 2, 4) + lax.rem(y + lax.rem(j, 4) + 2, 4)

    def far(k):
        return lax.rem(pix + pixes // 2 + (k + 1) // 2 * (1 - 2 * lax.rem(k, 2)), pixes)

    barrier = pltpu.get_barrier_semaphore()

    def tell_group(k):
        pl.semaphore_signal(barrier, inc=1, device_id={"ifg": lax.rem(me + k, GROUP)}, device_id_type=pl.DeviceIdType.MESH)

    def tell_pix(sem, other):
        pl.semaphore_signal(sem, inc=1, device_id={"pix": lax.rem(other, pixes)}, device_id_type=pl.DeviceIdType.MESH)

    def tell_along_z(sem, distance):
        tell_pix(sem, pix + 2 * distance)
        tell_pix(sem, pix + pixes - 2 * distance)

    read_inc = pltpu.make_async_copy(inc_hbm, inc, in_sem.at[0])
    read_inc.start()
    read_phase = pltpu.make_async_copy(phase_hbm, phase, in_sem.at[1])
    read_phase.start()
    read_weight = pltpu.make_async_copy(weight_hbm, weight, in_sem.at[2])
    read_weight.start()
    read_dates = pltpu.make_async_copy(dates_hbm, dates, in_sem.at[3])
    read_dates.start()
    pl.loop(1, GROUP)(tell_group)
    across = 2 * (pix // 2) + 1 - core
    tell_pix(barrier, across)
    tell_along_z(barrier, 1)
    tell_pix(barrier, across + 2)
    tell_pix(barrier, across + pixes - 2)

    iota[...] = lax.broadcasted_iota(jnp.int32, iota.shape, 0).astype(jnp.float32).astype(jnp.bfloat16)
    acc[...] = jnp.zeros_like(acc)
    scores[pix] = jnp.zeros(scores.shape[1:], scores.dtype)
    wrow[...] = jnp.zeros_like(wrow)
    rest16[...] = jnp.zeros_like(rest16)
    padded[...] = jnp.zeros_like(padded)

    read_inc.wait()
    read_phase.wait()
    read_weight.wait()
    read_dates.wait()
    padded[0:rows, :] = phase[...]
    wrow[0:1, 0 : weight.shape[1]] = weight[...]
    width = inc.shape[1]
    column = lax.broadcasted_iota(jnp.int32, (1, width), 1).astype(jnp.float32)
    column = column + jnp.floor((column + 0.5) * (1.0 / rows)) * (depth - rows)
    value = inc[...]
    plus = value == 1
    first = jnp.min(jnp.where(plus, column, 4096.0), axis=1, keepdims=True)
    second = jnp.max(jnp.where(plus, column, -1.0), axis=1, keepdims=True)
    long = jnp.sum(jnp.where(value == -1, column, 0.0), axis=1, keepdims=True)
    lane = lax.broadcasted_iota(jnp.int32, (inc.shape[0], LANES), 1)
    three = jnp.where(lane == 0, first, jnp.where(lane == 1, second, long))
    spot = 16 * lax.rem(me, 8)
    rest16[pl.ds(pl.multiple_of(spot, 16), 16), :] = three[LANES:]
    line = lax.broadcasted_iota(jnp.int32, (8, LANES), 0)
    for q, t, w in (
        (0, three[:LANES], wrow[:, :LANES]),
        (1, rest16[...], pltpu.roll(wrow[:, LANES:], spot, 1)),
    ):
        t = jnp.where(line < 3, jnp.transpose(t)[0:8], 0.0)
        idx[:, q * LANES : (q + 1) * LANES] = jnp.where(line == 3, jnp.broadcast_to(w[0:1], t.shape), t)

    pl.semaphore_wait(barrier, GROUP + 4)
    tell_along_z(near1, 1)

    def put(src, dst, send, recv, device):
        @pl.when(device != me)
        def _():
            pltpu.make_async_remote_copy(
                src_ref=src, dst_ref=dst, send_sem=send, recv_sem=recv,
                device_id={"ifg": device}, device_id_type=pl.DeviceIdType.MESH,
            ).start()

        @pl.when(device == me)
        def _():
            pltpu.make_async_copy(src, dst, recv).start()

    def took(ref, sem):
        pltpu.make_async_copy(ref, ref, sem).wait()

    def to_shares(body):
        @pl.loop(0, GROUP)
        def _(j):
            device = peer(j)
            their = rank_of(device, core)

            @pl.when(their < 3)
            def _():
                body(device, pl.multiple_of((3 * (device // 4) + their) * LANES, LANES))

    to_shares(lambda d, at: put(idx, idxs.at[me], idx_s.at[d], idx_r.at[me], d))
    to_shares(lambda d, at: put(padded.at[:, pl.ds(at, LANES)], ph.at[me], ph_s.at[d], ph_r.at[me], d))

    pl.semaphore_wait(near1, 2)
    tell_along_z(near2, 2)
    pl.semaphore_wait(near2, 2)
    tell_along_z(near4, 4)

    def pair(j):
        return lax.rem(me // 2 + j, GROUP // 2)

    def build(j):
        t = tiles[j]
        at = iota[...]
        one = jnp.ones(at.shape, jnp.bfloat16)
        for b in range(GROUP):
            rel = (t - float(b * depth)).astype(jnp.bfloat16)
            both = jnp.logical_or(at == rel[0:1], at == rel[1:2])
            signed = jnp.where(at == rel[2:3], -one, jnp.where(both, one, jnp.zeros_like(one)))
            inct[j, b * depth : (b + 1) * depth, :] = signed

    def finish(j):
        sine, loss = sin_and_loss(clo[...])
        acc[...] += loss * tiles[j, 3:4, :]
        wb[j] = jnp.transpose(sine).astype(jnp.bfloat16)

    def send_rows(j):
        if j < GROUP // 2:
            for q in range(2):
                d = 2 * pair(j) + q
                put(wb.at[j, pl.ds(q * LANES, LANES)], res_ref.at[pl.ds(0, LANES), my_lanes], res_s.at[d], res_r.at[share], d)
            return

        @pl.loop(0, GROUP)
        def _(k):
            d = peer(k)
            put(
                wb.at[j, pl.ds(pl.multiple_of(16 * d, 16), 16)],
                res_ref.at[pl.ds(LANES, 16), my_lanes], lef_s.at[d], lef_r.at[share], d,
            )

    @pl.when(active)
    def _():
        @pl.loop(0, GROUP)
        def _(d):
            took(idxs.at[d], idx_r.at[d])

        for j in range(GROUP // 2):
            for q in range(2):
                tiles[j, :, q * LANES : (q + 1) * LANES] = idxs[2 * pair(j) + q, :, 0:LANES]
        for q in range(2):
            rest = idxs[8 * q, :, LANES:]
            for i in range(1, 8):
                rest = rest + idxs[8 * q + i, :, LANES:]
            tiles[GROUP // 2, :, q * LANES : (q + 1) * LANES] = rest
        build(0)

        for half in range(2):
            for d in range(8 * half, 8 * half + 8):
                took(ph.at[d], ph_r.at[d])
            block = ph[8 * half : 8 * half + 8].reshape(8 * depth, LANES)
            pht[:, 8 * depth * half : 8 * depth * (half + 1)] = jnp.transpose(block.astype(jnp.float32)).astype(jnp.bfloat16)

        for j in range(steps):
            closure = jnp.dot(pht[...], inct[j], preferred_element_type=jnp.float32)
            if j > 0:
                finish(j - 1)
            if j + 1 < steps:
                build(j + 1)
            clo[...] = closure
            if j > 0:
                send_rows(j - 1)
        finish(steps - 1)

        total = tiles[0, 3:4, :]
        for j in range(1, steps):
            total = total + tiles[j, 3:4, :]
        both = acc[:, 0:LANES] + acc[:, LANES:]
        misfit = jnp.sum(jnp.transpose(both), axis=0, keepdims=True)
        scores[pix] = misfit / jnp.sum(total, axis=1, keepdims=True)

    pl.semaphore_wait(near4, 2)

    @pl.loop(0, pixes - 1)
    def _(k):
        other = far(k)
        pltpu.make_async_remote_copy(
            src_ref=scores.at[pix], dst_ref=scores.at[pix], send_sem=pix_s.at[other], recv_sem=pix_r.at[pix],
            device_id={"pix": other}, device_id_type=pl.DeviceIdType.MESH,
        ).start()

    @pl.when(active)
    def _():
        send_rows(steps - 1)

        @pl.loop(0, 4)
        def _(j):
            c = lax.rem(x + 2 + j, 4)
            at = pl.ds(pl.multiple_of(c * 4 * depth, 4 * depth), 4 * depth)
            corr = jnp.zeros((4 * depth, LANES), jnp.float32)
            for p in range(steps):
                corr = corr + jnp.dot(inct[p, at, :], wb[p], preferred_element_type=jnp.float32)
            cb[pl.ds(4 * c, 4)] = corr.astype(jnp.bfloat16).reshape(4, depth, LANES)
            for q in range(4):
                d = 4 * c + q
                put(cb.at[d], cor_ref.at[:, my_lanes], cor_s.at[d], cor_r.at[share], d)

    @pl.loop(0, pixes - 1)
    def _(k):
        other = far(k)
        took(scores.at[other], pix_r.at[other])

    fin_out[0:1] = scores[pix]
    fin_out[1:2] = jnp.sum(scores[...], axis=0)
    slot = jnp.where(active, share, 12 + x)

    @pl.loop(0, GROUP)
    def _(k):
        d = peer(k)
        put(fin_out, fin.at[slot], fin_s.at[d], fin_r.at[slot], d)

    @pl.loop(0, pixes - 1)
    def _(k):
        took(scores.at[pix], pix_s.at[far(k)])

    @pl.loop(1, GROUP)
    def _(k):
        d = lax.rem(me + k, GROUP)

        @pl.when(rank_of(d, core) < 3)
        def _():
            took(idxs.at[0], idx_s.at[d])
            took(ph.at[0], ph_s.at[d])

        @pl.when(active)
        def _():
            took(wb.at[0, pl.ds(0, LANES)], res_s.at[d])
            took(wb.at[0, pl.ds(0, 16)], lef_s.at[d])
            took(cb.at[0], cor_s.at[d])

    @pl.loop(0, 12)
    def _(s):
        lanes = pl.ds(pl.multiple_of(s * LANES, LANES), LANES)
        took(res_ref.at[pl.ds(0, LANES), lanes], res_r.at[s])
        took(res_ref.at[pl.ds(LANES, 16), lanes], lef_r.at[s])
        took(cor_ref.at[:, lanes], cor_r.at[s])

    span = (dates[1:2] - dates[0:1]).astype(jnp.float32)
    damp = jnp.concatenate([1.0 / (2.0 + span), jnp.zeros((1, LANES - rows), jnp.float32)], axis=1)
    damp = jnp.transpose(jnp.broadcast_to(damp, (LANES, LANES)))[:rows]

    @pl.loop(0, 12)
    def _(s):
        lanes = pl.ds(pl.multiple_of(s * LANES, LANES), LANES)
        residual_ref[:, lanes] = res_ref[:, lanes].astype(jnp.float32)
        corrected_ref[:, lanes] = phase[:, lanes].astype(jnp.float32) - cor_ref[0:rows, lanes].astype(jnp.float32) * damp

    @pl.loop(1, GROUP)
    def _(k):
        took(fin_out, fin_s.at[lax.rem(me + k, GROUP)])

    @pl.loop(0, GROUP)
    def _(s):
        took(fin.at[s], fin_r.at[s])

    everything = jnp.sum(jnp.sum(fin[...], axis=0)[1:2], axis=1, keepdims=True)
    for s in range(12):
        rel_ref[:, s * LANES : (s + 1) * LANES] = fin[s, 0:1] / (everything / all_pixels)


def local(phase, incidence, triplet_weight, date_pairs):
    rows, pixel_count = phase.shape
    depth = -(-rows // 16) * 16
    triplets = incidence.shape[0]
    pairs = GROUP // 2 + 1
    hbm = pl.BlockSpec(memory_space=pltpu.HBM)
    vmem = pl.BlockSpec(memory_space=pltpu.VMEM)
    pixes = lax.axis_size("pix")
    sems = [pltpu.SemaphoreType.DMA((GROUP,))] * 12
    operands = (phase, incidence, triplet_weight.reshape(1, triplets), date_pairs.T)
    operands = [pltpu.with_memory_space_constraint(a, pltpu.HBM) for a in operands]
    residual, relative, corrected = pl.pallas_call(
        functools.partial(kernel, pixes * pixel_count),
        out_shape=(
            jax.ShapeDtypeStruct((triplets, pixel_count), jnp.float32),
            jax.ShapeDtypeStruct((1, pixel_count), jnp.float32),
            jax.ShapeDtypeStruct((rows, pixel_count), jnp.float32),
        ),
        in_specs=[hbm] * 4,
        out_specs=[vmem] * 3,
        scratch_shapes=[
            pltpu.VMEM(incidence.shape, jnp.int32),
            pltpu.VMEM(phase.shape, jnp.bfloat16),
            pltpu.VMEM((1, triplets), jnp.float32),
            pltpu.VMEM((2, rows), jnp.int32),
            pltpu.VMEM((triplets, pixel_count), jnp.bfloat16),
            pltpu.VMEM((depth, pixel_count), jnp.bfloat16),
            pltpu.VMEM((8, 2 * LANES), jnp.float32),
            pltpu.VMEM((LANES, LANES), jnp.float32),
            pltpu.VMEM((8, 2 * LANES), jnp.float32),
            pltpu.VMEM((depth, pixel_count), jnp.bfloat16),
            pltpu.VMEM((GROUP, depth, LANES), jnp.bfloat16),
            pltpu.VMEM((LANES, GROUP * depth), jnp.bfloat16),
            pltpu.VMEM((GROUP, 8, 2 * LANES), jnp.float32),
            pltpu.VMEM((pairs, 8, 2 * LANES), jnp.float32),
            pltpu.VMEM((pairs, GROUP * depth, 2 * LANES), jnp.bfloat16),
            pltpu.VMEM((depth, 2 * LANES), jnp.bfloat16),
            pltpu.VMEM((LANES, 2 * LANES), jnp.float32),
            pltpu.VMEM((pairs, 2 * LANES, LANES), jnp.bfloat16),
            pltpu.VMEM((GROUP, depth, LANES), jnp.bfloat16),
            pltpu.VMEM((LANES, 2 * LANES), jnp.float32),
            pltpu.VMEM((pixes, 1, LANES), jnp.float32),
            pltpu.VMEM((2, LANES), jnp.float32),
            pltpu.VMEM((GROUP, 2, LANES), jnp.float32),
            pltpu.SemaphoreType.DMA((4,)),
            *sems,
            pltpu.SemaphoreType.DMA((pixes,)),
            pltpu.SemaphoreType.DMA((pixes,)),
            pltpu.SemaphoreType.REGULAR,
            pltpu.SemaphoreType.REGULAR,
            pltpu.SemaphoreType.REGULAR,
        ],
        compiler_params=pltpu.CompilerParams(collective_id=0, has_side_effects=True, vmem_limit_bytes=VMEM),
    )(*operands)
    return (residual, relative.reshape(pixel_count), corrected)


def solution(mesh):
    return jax.shard_map(
        local,
        mesh=mesh,
        in_specs=(P("ifg", "pix"), P("ifg", None), P("ifg"), P("ifg", None)),
        out_specs=(P("ifg", "pix"), P("pix"), P("ifg", "pix")),
        check_vma=False,
    )
```

```python
import functools

import jax
import jax.numpy as jnp
from jax import lax
from jax.experimental import pallas as pl
from jax.experimental.pallas import tpu as pltpu
from jax.sharding import PartitionSpec as P

GROUP = 16
LANES = 128
VMEM = 16 * 1024 * 1024
INV_2PI = 0.15915494309189535
TWO_PI_HI = 6.28125
TWO_PI_LO = 1.9353071795864769e-3
SIN = (-0.041666642741103474, 0.000520813580633296, -3.094783609930149e-06, 1.0156463124188801e-08)
COS = (-0.12499999887388552, 0.0026041650454957602, -2.170063047895746e-05, 9.672611781418933e-08, -2.5465921654786513e-10)


def poly(coefs, z):
    out = z * coefs[-1] + coefs[-2]
    for c in coefs[-3::-1]:
        out = out * z + c
    return out


def sin_and_twice_loss(x):
    k = jnp.round(x * INV_2PI)
    r = (x - k * TWO_PI_HI) - k * TWO_PI_LO
    z = r * r
    sine = r + (r * z) * poly(SIN, z)
    cosine = 1.0 + z * poly(COS, z)
    return sine * cosine, sine * sine


def rank_of(device, core):
    return lax.rem(lax.rem(device, 4) - device // 4 - 2 * core + 7, 4)


def kernel(
    all_pixels,
    phase_hbm, inc_hbm, weight_hbm, dates_hbm, residual_ref, rel_ref, corrected_ref,
    inc, phase, weight, dates, res_ref, cor_ref, idx, rest16, wrow, padded, ph, pht, idxs, tiles, inct, iota, clo, wb, cb, acc, scores, fin_out, fin,
    in_sem, ph_r, idx_s, idx_r, ph_s, res_s, res_r, lef_s, cor_s, cor_r, fin_s, fin_r, pix_s, pix_r,
    near1, near2, near4,
):
    me = lax.axis_index("ifg")
    pix = lax.axis_index("pix")
    x, y = me // 4, lax.rem(me, 4)
    core = lax.rem(pix, 2)
    rank = rank_of(me, core)
    active = rank < 3
    share = 3 * x + rank
    my_lanes = pl.ds(pl.multiple_of(share * LANES, LANES), LANES)
    rows = phase.shape[0]
    depth = padded.shape[0]
    pixes = scores.shape[0]
    steps = GROUP // 2 + 1

    def peer(j):
        return 4 * lax.rem(x + j // 4 + 2, 4) + lax.rem(y + lax.rem(j, 4) + 2, 4)

    def far(k):
        return lax.rem(pix + pixes // 2 + (k + 1) // 2 * (1 - 2 * lax.rem(k, 2)), pixes)

    barrier = pltpu.get_barrier_semaphore()

    def tell_group(k):
        pl.semaphore_signal(barrier, inc=1, device_id={"ifg": lax.rem(me + k, GROUP)}, device_id_type=pl.DeviceIdType.MESH)

    def tell_pix(sem, other):
        pl.semaphore_signal(sem, inc=1, device_id={"pix": lax.rem(other, pixes)}, device_id_type=pl.DeviceIdType.MESH)

    def tell_along_z(sem, distance):
        tell_pix(sem, pix + 2 * distance)
        tell_pix(sem, pix + pixes - 2 * distance)

    read_inc = pltpu.make_async_copy(inc_hbm, inc, in_sem.at[0])
    read_inc.start()
    read_phase = pltpu.make_async_copy(phase_hbm, phase, in_sem.at[1])
    read_phase.start()
    read_weight = pltpu.make_async_copy(weight_hbm, weight, in_sem.at[2])
    read_weight.start()
    read_dates = pltpu.make_async_copy(dates_hbm, dates, in_sem.at[3])
    read_dates.start()
    pl.loop(1, GROUP)(tell_group)
    across = 2 * (pix // 2) + 1 - core
    tell_pix(barrier, across)
    tell_along_z(barrier, 1)
    tell_pix(barrier, across + 2)
    tell_pix(barrier, across + pixes - 2)

    iota[...] = lax.broadcasted_iota(jnp.int32, iota.shape, 0).astype(jnp.float32).astype(jnp.bfloat16)
    acc[...] = jnp.zeros_like(acc)
    scores[pix] = jnp.zeros(scores.shape[1:], scores.dtype)
    wrow[...] = jnp.zeros_like(wrow)
    rest16[...] = jnp.zeros_like(rest16)
    padded[...] = jnp.zeros_like(padded)

    read_inc.wait()
    read_phase.wait()
    read_weight.wait()
    read_dates.wait()
    padded[0:rows, :] = phase[...]
    wrow[0:1, 0 : weight.shape[1]] = weight[...]
    width = inc.shape[1]
    column = lax.broadcasted_iota(jnp.int32, (1, width), 1).astype(jnp.float32)
    value = inc[...]
    plus = value == 1
    first = jnp.min(jnp.where(plus, column, 4096.0), axis=1, keepdims=True)
    second = jnp.max(jnp.where(plus, column, -1.0), axis=1, keepdims=True)
    long = jnp.sum(jnp.where(value == -1, column, 0.0), axis=1, keepdims=True)
    lane = lax.broadcasted_iota(jnp.int32, (inc.shape[0], LANES), 1)
    three = jnp.where(lane == 0, first, jnp.where(lane == 1, second, long))
    spot = 16 * lax.rem(me, 8)
    rest16[pl.ds(pl.multiple_of(spot, 16), 16), :] = three[LANES:]
    here = lax.broadcasted_iota(jnp.int32, (8, LANES), 1) // 16 == lax.rem(me, 8)
    for q, t, w in (
        (0, three[:LANES], wrow[:, :LANES]),
        (1, rest16[...], pltpu.roll(wrow[:, LANES:], spot, 1)),
    ):
        t = jnp.transpose(t)[0:8]
        block = jnp.floor((t + 0.5) * (1.0 / rows))
        message = jnp.concatenate([(t - block * rows)[0:3], block[0:3], w[0:1], jnp.zeros_like(w[0:1])], axis=0)
        idx[:, q * LANES : (q + 1) * LANES] = jnp.where(jnp.logical_or(q == 0, here), message, 0.0)

    pl.semaphore_wait(barrier, GROUP + 4)
    tell_along_z(near1, 1)

    def put(src, dst, send, recv, device):
        @pl.when(device != me)
        def _():
            pltpu.make_async_remote_copy(
                src_ref=src, dst_ref=dst, send_sem=send, recv_sem=recv,
                device_id={"ifg": device}, device_id_type=pl.DeviceIdType.MESH,
            ).start()

        @pl.when(device == me)
        def _():
            pltpu.make_async_copy(src, dst, recv).start()

    def took(ref, sem):
        pltpu.make_async_copy(ref, ref, sem).wait()

    def to_shares(body):
        @pl.loop(0, GROUP)
        def _(j):
            device = peer(j)
            their = rank_of(device, core)

            @pl.when(their < 3)
            def _():
                body(device, pl.multiple_of((3 * (device // 4) + their) * LANES, LANES))

    to_shares(lambda d, at: put(idx, idxs.at[me], idx_s, idx_r, d))
    to_shares(lambda d, at: put(padded.at[:, pl.ds(at, LANES)], ph.at[me], ph_s, ph_r.at[me // 8], d))

    pl.semaphore_wait(near1, 2)
    tell_along_z(near2, 2)
    pl.semaphore_wait(near2, 2)
    tell_along_z(near4, 4)

    def pair(j):
        return lax.rem(me // 2 + j, GROUP // 2)

    def build(j):
        t = tiles[j]
        at = iota[...]
        lines = []
        blocks = []
        for i in range(3):
            row = jnp.broadcast_to(t[i : i + 1], at.shape).astype(jnp.bfloat16)
            lines.append(jnp.where(at == row, jnp.full_like(at, -1.0 if i == 2 else 1.0), jnp.zeros_like(at)))
            blocks.append(jnp.broadcast_to(t[3 + i : 4 + i], (16, at.shape[1])).astype(jnp.bfloat16))
        one = jnp.ones_like(blocks[0])
        for b in range(GROUP):
            inside = [jnp.where(v == one * b, one, jnp.zeros_like(one)) for v in blocks]
            for g in range(depth // 16):
                terms = [v * line[16 * g : 16 * g + 16] for v, line in zip(inside, lines)]
                inct[j, b * depth + 16 * g : b * depth + 16 * g + 16, :] = terms[0] + terms[1] + terms[2]

    def finish(j):
        sine, loss = sin_and_twice_loss(clo[...])
        acc[...] += loss * (0.5 * tiles[j, 6:7, :])
        wb[j] = jnp.transpose(sine).astype(jnp.bfloat16)

    def send_rows(j):
        if j < GROUP // 2:
            for q in range(2):
                d = 2 * pair(j) + q
                put(wb.at[j, pl.ds(q * LANES, LANES)], res_ref.at[pl.ds(0, LANES), my_lanes], res_s, res_r, d)
            return

        @pl.loop(0, GROUP)
        def _(k):
            d = peer(k)
            put(
                wb.at[j, pl.ds(pl.multiple_of(16 * d, 16), 16)],
                res_ref.at[pl.ds(LANES, 16), my_lanes], lef_s, res_r, d,
            )

    @pl.when(active)
    def _():
        took(idxs, idx_r)

        for j in range(GROUP // 2):
            for q in range(2):
                tiles[j, :, q * LANES : (q + 1) * LANES] = idxs[2 * pair(j) + q, :, 0:LANES]
        for q in range(2):
            rest = idxs[8 * q, :, LANES:]
            for i in range(1, 8):
                rest = rest + idxs[8 * q + i, :, LANES:]
            tiles[GROUP // 2, :, q * LANES : (q + 1) * LANES] = rest
        build(0)

        for half in range(2):
            took(ph.at[pl.ds(8 * half, 8)], ph_r.at[half])
            block = ph[8 * half : 8 * half + 8].reshape(8 * depth, LANES)
            pht[:, 8 * depth * half : 8 * depth * (half + 1)] = jnp.transpose(block.astype(jnp.float32)).astype(jnp.bfloat16)

        for j in range(steps):
            closure = jnp.dot(pht[...], inct[j], preferred_element_type=jnp.float32)
            if j > 0:
                finish(j - 1)
            if j + 1 < steps:
                build(j + 1)
            clo[...] = closure
            if j > 0:
                send_rows(j - 1)
        finish(steps - 1)

        total = tiles[0, 6:7, :]
        for j in range(1, steps):
            total = total + tiles[j, 6:7, :]
        both = acc[:, 0:LANES] + acc[:, LANES:]
        misfit = jnp.sum(jnp.transpose(both), axis=0, keepdims=True)
        scores[pix] = misfit / jnp.sum(total, axis=1, keepdims=True)

    pl.semaphore_wait(near4, 2)

    @pl.loop(0, pixes - 1)
    def _(k):
        other = far(k)
        pltpu.make_async_remote_copy(
            src_ref=scores.at[pix], dst_ref=scores.at[pix], send_sem=pix_s, recv_sem=pix_r,
            device_id={"pix": other}, device_id_type=pl.DeviceIdType.MESH,
        ).start()

    @pl.when(active)
    def _():
        send_rows(steps - 1)

        @pl.loop(0, 4)
        def _(j):
            c = lax.rem(x + 2 + j, 4)
            at = pl.ds(pl.multiple_of(c * 4 * depth, 4 * depth), 4 * depth)
            corr = jnp.zeros((4 * depth, LANES), jnp.float32)
            for p in range(steps):
                corr = corr + jnp.dot(inct[p, at, :], wb[p], preferred_element_type=jnp.float32)
            cb[pl.ds(4 * c, 4)] = corr.astype(jnp.bfloat16).reshape(4, depth, LANES)
            for q in range(4):
                d = 4 * c + q
                put(cb.at[d], cor_ref.at[:, my_lanes], cor_s, cor_r, d)

    took(scores.at[pl.ds(0, pixes - 1)], pix_r)

    fin_out[0:1] = scores[pix]
    fin_out[1:2] = jnp.sum(scores[...], axis=0)
    slot = jnp.where(active, share, 12 + x)

    @pl.loop(0, GROUP)
    def _(k):
        d = peer(k)
        put(fin_out, fin.at[slot], fin_s, fin_r, d)

    others = GROUP - 1
    took(scores.at[pl.ds(0, pixes - 1)], pix_s)

    @pl.when(active)
    def _():
        took(idxs.at[pl.ds(0, 11)], idx_s)
        took(ph.at[pl.ds(0, 11)], ph_s)
        took(inct.at[0, pl.ds(0, others * LANES // 2)], res_s)
        took(wb.at[0, pl.ds(0, others * 16)], lef_s)
        took(cb.at[pl.ds(0, others)], cor_s)

    @pl.when(rank == 3)
    def _():
        took(idxs.at[pl.ds(0, 12)], idx_s)
        took(ph.at[pl.ds(0, 12)], ph_s)

    took(res_ref, res_r)
    took(cor_ref, cor_r)

    span = (dates[1:2] - dates[0:1]).astype(jnp.float32)
    damp = jnp.concatenate([1.0 / (2.0 + span), jnp.zeros((1, LANES - rows), jnp.float32)], axis=1)
    damp = jnp.transpose(jnp.broadcast_to(damp, (LANES, LANES)))[:rows]

    @pl.loop(0, 12)
    def _(s):
        lanes = pl.ds(pl.multiple_of(s * LANES, LANES), LANES)
        residual_ref[:, lanes] = res_ref[:, lanes].astype(jnp.float32)
        corrected_ref[:, lanes] = phase[:, lanes].astype(jnp.float32) - cor_ref[0:rows, lanes].astype(jnp.float32) * damp

    took(fin.at[pl.ds(0, others)], fin_s)
    took(fin, fin_r)

    everything = jnp.sum(jnp.sum(fin[...], axis=0)[1:2], axis=1, keepdims=True)
    for s in range(12):
        rel_ref[:, s * LANES : (s + 1) * LANES] = fin[s, 0:1] / (everything / all_pixels)


def local(phase, incidence, triplet_weight, date_pairs):
    rows, pixel_count = phase.shape
    depth = -(-rows // 16) * 16
    triplets = incidence.shape[0]
    pairs = GROUP // 2 + 1
    hbm = pl.BlockSpec(memory_space=pltpu.HBM)
    vmem = pl.BlockSpec(memory_space=pltpu.VMEM)
    pixes = lax.axis_size("pix")
    operands = (phase, incidence, triplet_weight.reshape(1, triplets), date_pairs.T)
    operands = [pltpu.with_memory_space_constraint(a, pltpu.HBM) for a in operands]
    residual, relative, corrected = pl.pallas_call(
        functools.partial(kernel, pixes * pixel_count),
        out_shape=(
            jax.ShapeDtypeStruct((triplets, pixel_count), jnp.float32),
            jax.ShapeDtypeStruct((1, pixel_count), jnp.float32),
            jax.ShapeDtypeStruct((rows, pixel_count), jnp.float32),
        ),
        in_specs=[hbm] * 4,
        out_specs=[vmem] * 3,
        scratch_shapes=[
            pltpu.VMEM(incidence.shape, jnp.int32),
            pltpu.VMEM(phase.shape, jnp.bfloat16),
            pltpu.VMEM((1, triplets), jnp.float32),
            pltpu.VMEM((2, rows), jnp.int32),
            pltpu.VMEM((triplets, pixel_count), jnp.bfloat16),
            pltpu.VMEM((depth, pixel_count), jnp.bfloat16),
            pltpu.VMEM((8, 2 * LANES), jnp.float32),
            pltpu.VMEM((LANES, LANES), jnp.float32),
            pltpu.VMEM((8, 2 * LANES), jnp.float32),
            pltpu.VMEM((depth, pixel_count), jnp.bfloat16),
            pltpu.VMEM((GROUP, depth, LANES), jnp.bfloat16),
            pltpu.VMEM((LANES, GROUP * depth), jnp.bfloat16),
            pltpu.VMEM((GROUP, 8, 2 * LANES), jnp.float32),
            pltpu.VMEM((pairs, 8, 2 * LANES), jnp.float32),
            pltpu.VMEM((pairs, GROUP * depth, 2 * LANES), jnp.bfloat16),
            pltpu.VMEM((depth, 2 * LANES), jnp.bfloat16),
            pltpu.VMEM((LANES, 2 * LANES), jnp.float32),
            pltpu.VMEM((pairs, 2 * LANES, LANES), jnp.bfloat16),
            pltpu.VMEM((GROUP, depth, LANES), jnp.bfloat16),
            pltpu.VMEM((LANES, 2 * LANES), jnp.float32),
            pltpu.VMEM((pixes, 1, LANES), jnp.float32),
            pltpu.VMEM((2, LANES), jnp.float32),
            pltpu.VMEM((GROUP, 2, LANES), jnp.float32),
            pltpu.SemaphoreType.DMA((4,)),
            pltpu.SemaphoreType.DMA((2,)),
            *[pltpu.SemaphoreType.DMA] * 12,
            *[pltpu.SemaphoreType.REGULAR] * 3,
        ],
        compiler_params=pltpu.CompilerParams(collective_id=0, has_side_effects=True, vmem_limit_bytes=VMEM),
    )(*operands)
    return (residual, relative.reshape(pixel_count), corrected)


def solution(mesh):
    return jax.shard_map(
        local,
        mesh=mesh,
        in_specs=(P("ifg", "pix"), P("ifg", None), P("ifg"), P("ifg", None)),
        out_specs=(P("ifg", "pix"), P("pix"), P("ifg", "pix")),
        check_vma=False,
    )
```

```python
import functools

import jax
import jax.numpy as jnp
from jax import lax
from jax.experimental import pallas as pl
from jax.experimental.pallas import tpu as pltpu
from jax.sharding import PartitionSpec as P

GROUP = 16
LANES = 128
VMEM = 16 * 1024 * 1024
INV_2PI = 0.15915494309189535
TWO_PI_HI = 6.28125
TWO_PI_LO = 1.9353071795864769e-3
SIN = (-0.041666642741103474, 0.000520813580633296, -3.094783609930149e-06, 1.0156463124188801e-08)
COS = (-0.12499999887388552, 0.0026041650454957602, -2.170063047895746e-05, 9.672611781418933e-08, -2.5465921654786513e-10)


def poly(coefs, z):
    out = z * coefs[-1] + coefs[-2]
    for c in coefs[-3::-1]:
        out = out * z + c
    return out


def sin_and_twice_loss(x):
    k = jnp.round(x * INV_2PI)
    r = (x - k * TWO_PI_HI) - k * TWO_PI_LO
    z = r * r
    sine = r + (r * z) * poly(SIN, z)
    cosine = 1.0 + z * poly(COS, z)
    return sine * cosine, sine * sine


def rank_of(device, core):
    return lax.rem(lax.rem(device, 4) - device // 4 - 2 * core + 7, 4)


def kernel(
    all_pixels,
    phase_hbm, inc_hbm, weight_hbm, dates_hbm, residual_ref, rel_ref, corrected_ref,
    inc, phase, weight, dates, res_ref, cor_ref, idx, rest16, wrow, padded, ph, pht, idxs, tiles, inct, iota, clo, wb, cb, acc, scores, fin_out, fin,
    in_sem, ph_r, idx_s, idx_r, ph_s, res_s, res_r, lef_s, cor_s, cor_r, fin_s, fin_r, pix_s, pix_r,
    near1, near2, near4,
):
    me = lax.axis_index("ifg")
    pix = lax.axis_index("pix")
    x, y = me // 4, lax.rem(me, 4)
    core = lax.rem(pix, 2)
    rank = rank_of(me, core)
    active = rank < 3
    share = 3 * x + rank
    my_lanes = pl.ds(pl.multiple_of(share * LANES, LANES), LANES)
    rows = phase.shape[0]
    depth = padded.shape[0]
    pixes = scores.shape[0]
    steps = GROUP // 2 + 1

    def peer(j):
        return 4 * lax.rem(x + j // 4 + 2, 4) + lax.rem(y + lax.rem(j, 4) + 2, 4)

    def far(k):
        return lax.rem(pix + pixes // 2 + (k + 1) // 2 * (1 - 2 * lax.rem(k, 2)), pixes)

    barrier = pltpu.get_barrier_semaphore()

    def tell_group(k):
        pl.semaphore_signal(barrier, inc=1, device_id={"ifg": lax.rem(me + k, GROUP)}, device_id_type=pl.DeviceIdType.MESH)

    def tell_pix(sem, other):
        pl.semaphore_signal(sem, inc=1, device_id={"pix": lax.rem(other, pixes)}, device_id_type=pl.DeviceIdType.MESH)

    def tell_along_z(sem, distance):
        tell_pix(sem, pix + 2 * distance)
        tell_pix(sem, pix + pixes - 2 * distance)

    read_inc = pltpu.make_async_copy(inc_hbm, inc, in_sem.at[0])
    read_inc.start()
    read_phase = pltpu.make_async_copy(phase_hbm, phase, in_sem.at[1])
    read_phase.start()
    read_weight = pltpu.make_async_copy(weight_hbm, weight, in_sem.at[2])
    read_weight.start()
    read_dates = pltpu.make_async_copy(dates_hbm, dates, in_sem.at[3])
    read_dates.start()
    pl.loop(1, GROUP)(tell_group)
    across = 2 * (pix // 2) + 1 - core
    tell_pix(barrier, across)
    tell_along_z(barrier, 1)
    tell_pix(barrier, across + 2)
    tell_pix(barrier, across + pixes - 2)

    iota[...] = lax.broadcasted_iota(jnp.int32, iota.shape, 0).astype(jnp.float32).astype(jnp.bfloat16)
    acc[...] = jnp.zeros_like(acc)
    scores[pix] = jnp.zeros(scores.shape[1:], scores.dtype)
    wrow[...] = jnp.zeros_like(wrow)
    rest16[...] = jnp.zeros_like(rest16)
    padded[...] = jnp.zeros_like(padded)

    read_inc.wait()
    read_phase.wait()
    read_weight.wait()
    read_dates.wait()
    padded[0:rows, :] = phase[...]
    wrow[0:1, 0 : weight.shape[1]] = weight[...]
    width = inc.shape[1]
    column = lax.broadcasted_iota(jnp.int32, (1, width), 1).astype(jnp.float32)
    value = inc[...]
    plus = value == 1
    first = jnp.min(jnp.where(plus, column, 4096.0), axis=1, keepdims=True)
    second = jnp.max(jnp.where(plus, column, -1.0), axis=1, keepdims=True)
    long = jnp.sum(jnp.where(value == -1, column, 0.0), axis=1, keepdims=True)
    lane = lax.broadcasted_iota(jnp.int32, (inc.shape[0], LANES), 1)
    three = jnp.where(lane == 0, first, jnp.where(lane == 1, second, long))
    spot = 16 * lax.rem(me, 8)
    rest16[pl.ds(pl.multiple_of(spot, 16), 16), :] = three[LANES:]
    here = lax.broadcasted_iota(jnp.int32, (8, LANES), 1) // 16 == lax.rem(me, 8)
    for q, t, w in (
        (0, three[:LANES], wrow[:, :LANES]),
        (1, rest16[...], pltpu.roll(wrow[:, LANES:], spot, 1)),
    ):
        t = jnp.transpose(t)[0:8]
        block = jnp.floor((t + 0.5) * (1.0 / rows))
        high = w[0:1].astype(jnp.bfloat16).astype(jnp.float32)
        message = jnp.concatenate([(t - block * rows)[0:3], block[0:3], high, w[0:1] - high], axis=0)
        idx[:, q * LANES : (q + 1) * LANES] = jnp.where(jnp.logical_or(q == 0, here), message, 0.0).astype(jnp.bfloat16)

    pl.semaphore_wait(barrier, GROUP + 4)
    tell_along_z(near1, 1)

    def put(src, dst, send, recv, device):
        @pl.when(device != me)
        def _():
            pltpu.make_async_remote_copy(
                src_ref=src, dst_ref=dst, send_sem=send, recv_sem=recv,
                device_id={"ifg": device}, device_id_type=pl.DeviceIdType.MESH,
            ).start()

        @pl.when(device == me)
        def _():
            pltpu.make_async_copy(src, dst, recv).start()

    def took(ref, sem):
        pltpu.make_async_copy(ref, ref, sem).wait()

    def to_shares(body):
        @pl.loop(0, GROUP)
        def _(j):
            device = peer(j)
            their = rank_of(device, core)

            @pl.when(their < 3)
            def _():
                body(device, pl.multiple_of((3 * (device // 4) + their) * LANES, LANES))

    to_shares(lambda d, at: put(idx, idxs.at[me], idx_s, idx_r, d))
    to_shares(lambda d, at: put(padded.at[:, pl.ds(at, LANES)], ph.at[me], ph_s, ph_r.at[me // 8], d))

    pl.semaphore_wait(near1, 2)
    tell_along_z(near2, 2)
    pl.semaphore_wait(near2, 2)
    tell_along_z(near4, 4)

    def pair(j):
        return lax.rem(me // 2 + j, GROUP // 2)

    def build(j):
        t = tiles[j]
        at = iota[...]
        lines = []
        blocks = []
        for i in range(3):
            row = jnp.broadcast_to(t[i : i + 1], at.shape).astype(jnp.bfloat16)
            lines.append(jnp.where(at == row, jnp.full_like(at, -1.0 if i == 2 else 1.0), jnp.zeros_like(at)))
            blocks.append(jnp.broadcast_to(t[3 + i : 4 + i], (16, at.shape[1])).astype(jnp.bfloat16))
        one = jnp.ones_like(blocks[0])
        for b in range(GROUP):
            inside = [jnp.where(v == one * b, one, jnp.zeros_like(one)) for v in blocks]
            for g in range(depth // 16):
                terms = [v * line[16 * g : 16 * g + 16] for v, line in zip(inside, lines)]
                inct[j, b * depth + 16 * g : b * depth + 16 * g + 16, :] = terms[0] + terms[1] + terms[2]

    def weights(j):
        return tiles[j, 6:7, :] + tiles[j, 7:8, :]

    def finish(j):
        sine, loss = sin_and_twice_loss(clo[...])
        acc[...] += loss * (0.5 * weights(j))
        wb[j] = jnp.transpose(sine).astype(jnp.bfloat16)

    def send_pair(j):
        for q in range(2):
            d = 2 * pair(j) + q
            put(wb.at[j, pl.ds(q * LANES, LANES)], res_ref.at[pl.ds(0, LANES), my_lanes], res_s, res_r, d)

    @pl.when(active)
    def _():
        took(idxs, idx_r)

        for j in range(GROUP // 2):
            for q in range(2):
                tiles[j, :, q * LANES : (q + 1) * LANES] = idxs[2 * pair(j) + q, :, 0:LANES].astype(jnp.float32)
        for q in range(2):
            rest = idxs[8 * q, :, LANES:].astype(jnp.float32)
            for i in range(1, 8):
                rest = rest + idxs[8 * q + i, :, LANES:].astype(jnp.float32)
            tiles[GROUP // 2, :, q * LANES : (q + 1) * LANES] = rest

        pl.loop(0, steps)(build)

        for half in range(2):
            took(ph.at[pl.ds(8 * half, 8)], ph_r.at[half])
            block = ph[8 * half : 8 * half + 8].reshape(8 * depth, LANES)
            pht[:, 8 * depth * half : 8 * depth * (half + 1)] = jnp.transpose(block.astype(jnp.float32)).astype(jnp.bfloat16)

        clo[...] = jnp.dot(pht[...], inct[0], preferred_element_type=jnp.float32)

        @pl.loop(1, steps)
        def _(j):
            closure = jnp.dot(pht[...], inct[j], preferred_element_type=jnp.float32)
            finish(j - 1)
            clo[...] = closure
            send_pair(j - 1)

        finish(steps - 1)

        total = weights(0)
        for j in range(1, steps):
            total = total + weights(j)
        both = acc[:, 0:LANES] + acc[:, LANES:]
        misfit = jnp.sum(jnp.transpose(both), axis=0, keepdims=True)
        scores[pix] = misfit / jnp.sum(total, axis=1, keepdims=True)

    pl.semaphore_wait(near4, 2)

    @pl.loop(0, pixes - 1)
    def _(k):
        other = far(k)
        pltpu.make_async_remote_copy(
            src_ref=scores.at[pix], dst_ref=scores.at[pix], send_sem=pix_s, recv_sem=pix_r,
            device_id={"pix": other}, device_id_type=pl.DeviceIdType.MESH,
        ).start()

    @pl.when(active)
    def _():
        @pl.loop(0, GROUP)
        def _(k):
            d = peer(k)
            put(
                wb.at[steps - 1, pl.ds(pl.multiple_of(16 * d, 16), 16)],
                res_ref.at[pl.ds(LANES, 16), my_lanes], lef_s, res_r, d,
            )

        @pl.loop(0, 4)
        def _(j):
            c = lax.rem(x + 2 + j, 4)
            at = pl.ds(pl.multiple_of(c * 4 * depth, 4 * depth), 4 * depth)
            corr = jnp.zeros((4 * depth, LANES), jnp.float32)
            for p in range(steps):
                corr = corr + jnp.dot(inct[p, at, :], wb[p], preferred_element_type=jnp.float32)
            cb[pl.ds(4 * c, 4)] = corr.astype(jnp.bfloat16).reshape(4, depth, LANES)
            for q in range(4):
                d = 4 * c + q
                put(cb.at[d], cor_ref.at[:, my_lanes], cor_s, cor_r, d)

    took(scores.at[pl.ds(0, pixes - 1)], pix_r)

    fin_out[0:1] = scores[pix]
    fin_out[1:2] = jnp.sum(scores[...], axis=0)
    slot = jnp.where(active, share, 12 + x)

    @pl.loop(0, GROUP)
    def _(k):
        d = peer(k)
        put(fin_out, fin.at[slot], fin_s, fin_r, d)

    others = GROUP - 1
    took(scores.at[pl.ds(0, pixes - 1)], pix_s)

    @pl.when(active)
    def _():
        took(idxs.at[pl.ds(0, 11)], idx_s)
        took(ph.at[pl.ds(0, 11)], ph_s)
        took(inct.at[0, pl.ds(0, others * LANES // 2)], res_s)
        took(wb.at[0, pl.ds(0, others * 16)], lef_s)
        took(cb.at[pl.ds(0, others)], cor_s)

    @pl.when(rank == 3)
    def _():
        took(idxs.at[pl.ds(0, 12)], idx_s)
        took(ph.at[pl.ds(0, 12)], ph_s)

    took(res_ref, res_r)
    took(cor_ref, cor_r)

    span = (dates[1:2] - dates[0:1]).astype(jnp.float32)
    damp = jnp.concatenate([1.0 / (2.0 + span), jnp.zeros((1, LANES - rows), jnp.float32)], axis=1)
    damp = jnp.transpose(jnp.broadcast_to(damp, (LANES, LANES)))[:rows]

    @pl.loop(0, 12)
    def _(s):
        lanes = pl.ds(pl.multiple_of(s * LANES, LANES), LANES)
        residual_ref[:, lanes] = res_ref[:, lanes].astype(jnp.float32)
        corrected_ref[:, lanes] = phase[:, lanes].astype(jnp.float32) - cor_ref[0:rows, lanes].astype(jnp.float32) * damp

    took(fin.at[pl.ds(0, others)], fin_s)
    took(fin, fin_r)

    everything = jnp.sum(jnp.sum(fin[...], axis=0)[1:2], axis=1, keepdims=True)
    for s in range(12):
        rel_ref[:, s * LANES : (s + 1) * LANES] = fin[s, 0:1] / (everything / all_pixels)


def store(*refs):
    n = len(refs) // 2
    sems = refs[-1]
    flat = [r.at[0] if r.shape[0] == 1 else r for r in refs[:n]]
    copies = [pltpu.make_async_copy(flat[i], refs[n + i], sems.at[i]) for i in range(n)]
    for copy in copies:
        copy.start()
    for copy in copies:
        copy.wait()


def local(phase, incidence, triplet_weight, date_pairs):
    rows, pixel_count = phase.shape
    depth = -(-rows // 16) * 16
    triplets = incidence.shape[0]
    pairs = GROUP // 2 + 1
    hbm = pl.BlockSpec(memory_space=pltpu.HBM)
    vmem = pl.BlockSpec(memory_space=pltpu.VMEM)
    pixes = lax.axis_size("pix")
    operands = (phase, incidence, triplet_weight.reshape(1, triplets), date_pairs.T)
    operands = [pltpu.with_memory_space_constraint(a, pltpu.HBM) for a in operands]
    residual, relative, corrected = pl.pallas_call(
        functools.partial(kernel, pixes * pixel_count),
        out_shape=(
            jax.ShapeDtypeStruct((triplets, pixel_count), jnp.float32),
            jax.ShapeDtypeStruct((1, pixel_count), jnp.float32),
            jax.ShapeDtypeStruct((rows, pixel_count), jnp.float32),
        ),
        in_specs=[hbm] * 4,
        out_specs=[vmem] * 3,
        scratch_shapes=[
            pltpu.VMEM(incidence.shape, jnp.int32),
            pltpu.VMEM(phase.shape, jnp.bfloat16),
            pltpu.VMEM((1, triplets), jnp.float32),
            pltpu.VMEM((2, rows), jnp.int32),
            pltpu.VMEM((triplets, pixel_count), jnp.bfloat16),
            pltpu.VMEM((depth, pixel_count), jnp.bfloat16),
            pltpu.VMEM((8, 2 * LANES), jnp.bfloat16),
            pltpu.VMEM((LANES, LANES), jnp.float32),
            pltpu.VMEM((8, 2 * LANES), jnp.float32),
            pltpu.VMEM((depth, pixel_count), jnp.bfloat16),
            pltpu.VMEM((GROUP, depth, LANES), jnp.bfloat16),
            pltpu.VMEM((LANES, GROUP * depth), jnp.bfloat16),
            pltpu.VMEM((GROUP, 8, 2 * LANES), jnp.bfloat16),
            pltpu.VMEM((pairs, 8, 2 * LANES), jnp.float32),
            pltpu.VMEM((pairs, GROUP * depth, 2 * LANES), jnp.bfloat16),
            pltpu.VMEM((depth, 2 * LANES), jnp.bfloat16),
            pltpu.VMEM((LANES, 2 * LANES), jnp.float32),
            pltpu.VMEM((pairs, 2 * LANES, LANES), jnp.bfloat16),
            pltpu.VMEM((GROUP, depth, LANES), jnp.bfloat16),
            pltpu.VMEM((LANES, 2 * LANES), jnp.float32),
            pltpu.VMEM((pixes, 1, LANES), jnp.float32),
            pltpu.VMEM((2, LANES), jnp.float32),
            pltpu.VMEM((GROUP, 2, LANES), jnp.float32),
            pltpu.SemaphoreType.DMA((4,)),
            pltpu.SemaphoreType.DMA((2,)),
            *[pltpu.SemaphoreType.DMA] * 12,
            *[pltpu.SemaphoreType.REGULAR] * 3,
        ],
        compiler_params=pltpu.CompilerParams(collective_id=0, has_side_effects=True, vmem_limit_bytes=VMEM),
    )(*operands)
    return pl.pallas_call(
        store,
        out_shape=(
            jax.ShapeDtypeStruct(residual.shape, jnp.float32),
            jax.ShapeDtypeStruct((pixel_count,), jnp.float32),
            jax.ShapeDtypeStruct(corrected.shape, jnp.float32),
        ),
        in_specs=[pl.BlockSpec(memory_space=pl.ANY)] * 3,
        out_specs=[hbm] * 3,
        scratch_shapes=[pltpu.SemaphoreType.DMA((3,))],
        compiler_params=pltpu.CompilerParams(vmem_limit_bytes=1024 * 1024),
    )(residual, relative, corrected)


def solution(mesh):
    return jax.shard_map(
        local,
        mesh=mesh,
        in_specs=(P("ifg", "pix"), P("ifg", None), P("ifg"), P("ifg", None)),
        out_specs=(P("ifg", "pix"), P("pix"), P("ifg", "pix")),
        check_vma=False,
    )
```

```python
import functools

import jax
import jax.numpy as jnp
from jax import lax
from jax.experimental import pallas as pl
from jax.experimental.pallas import tpu as pltpu
from jax.sharding import PartitionSpec as P

GROUP = 16
LANES = 128
VMEM = 16 * 1024 * 1024
INV_2PI = 0.15915494309189535
TWO_PI_HI = 6.28125
TWO_PI_LO = 1.9353071795864769e-3
SIN = (-0.041666642741103474, 0.000520813580633296, -3.094783609930149e-06, 1.0156463124188801e-08)
COS = (-0.12499999887388552, 0.0026041650454957602, -2.170063047895746e-05, 9.672611781418933e-08, -2.5465921654786513e-10)


def poly(coefs, z):
    out = z * coefs[-1] + coefs[-2]
    for c in coefs[-3::-1]:
        out = out * z + c
    return out


def sin_and_twice_loss(x):
    k = jnp.round(x * INV_2PI)
    r = (x - k * TWO_PI_HI) - k * TWO_PI_LO
    z = r * r
    sine = r + (r * z) * poly(SIN, z)
    cosine = 1.0 + z * poly(COS, z)
    return sine * cosine, sine * sine


def rank_of(device, core):
    return lax.rem(lax.rem(device, 4) + device // 4 + 2 * core, 4)


def kernel(
    all_pixels,
    phase_hbm, inc_hbm, weight_hbm, dates_hbm, residual_ref, rel_ref, corrected_ref,
    inc, phase, weight, dates, res_ref, cor_ref, idx, rest16, wrow, padded, ph, pht, idxs, tiles, inct, iota, clo, wb, cb, acc, scores, fin_out, fin,
    in_sem, ph_r, idx_r, idx_s, ph_s, res_s, res_r, lef_s, cor_s, cor_r, fin_s, fin_r, pix_s, pix_r,
    near1, near2, near4,
):
    me = lax.axis_index("ifg")
    pix = lax.axis_index("pix")
    x, y = me // 4, lax.rem(me, 4)
    core = lax.rem(pix, 2)
    rank = rank_of(me, core)
    active = rank < 3
    share = 3 * x + rank
    my_lanes = pl.ds(pl.multiple_of(share * LANES, LANES), LANES)
    rows = phase.shape[0]
    depth = padded.shape[0]
    pixes = scores.shape[0]
    steps = GROUP // 2 + 1

    def peer(j):
        return 4 * lax.rem(x + j // 4 + 2, 4) + lax.rem(y + lax.rem(j, 4) + 2, 4)

    def far(k):
        return lax.rem(pix + pixes // 2 + (k + 1) // 2 * (1 - 2 * lax.rem(k, 2)), pixes)

    barrier = pltpu.get_barrier_semaphore()

    def tell_group(k):
        pl.semaphore_signal(barrier, inc=1, device_id={"ifg": lax.rem(me + k, GROUP)}, device_id_type=pl.DeviceIdType.MESH)

    def tell_pix(sem, other):
        pl.semaphore_signal(sem, inc=1, device_id={"pix": lax.rem(other, pixes)}, device_id_type=pl.DeviceIdType.MESH)

    def tell_along_z(sem, distance):
        tell_pix(sem, pix + 2 * distance)
        tell_pix(sem, pix + pixes - 2 * distance)

    read_inc = pltpu.make_async_copy(inc_hbm, inc, in_sem.at[0])
    read_inc.start()
    read_phase = pltpu.make_async_copy(phase_hbm, phase, in_sem.at[1])
    read_phase.start()
    read_weight = pltpu.make_async_copy(weight_hbm, weight, in_sem.at[2])
    read_weight.start()
    read_dates = pltpu.make_async_copy(dates_hbm, dates, in_sem.at[3])
    read_dates.start()
    pl.loop(1, GROUP)(tell_group)
    across = 2 * (pix // 2) + 1 - core
    tell_pix(barrier, across)
    tell_along_z(barrier, 1)
    tell_pix(barrier, across + 2)
    tell_pix(barrier, across + pixes - 2)

    iota[...] = lax.broadcasted_iota(jnp.int32, iota.shape, 0).astype(jnp.float32).astype(jnp.bfloat16)
    acc[...] = jnp.zeros_like(acc)
    scores[pix] = jnp.zeros(scores.shape[1:], scores.dtype)
    wrow[...] = jnp.zeros_like(wrow)
    rest16[...] = jnp.zeros_like(rest16)
    padded[...] = jnp.zeros_like(padded)

    read_inc.wait()
    read_phase.wait()
    read_weight.wait()
    read_dates.wait()
    padded[0:rows, :] = phase[...]
    wrow[0:1, 0 : weight.shape[1]] = weight[...]
    width = inc.shape[1]
    column = lax.broadcasted_iota(jnp.int32, (1, width), 1).astype(jnp.float32)
    value = inc[...]
    plus = value == 1
    first = jnp.min(jnp.where(plus, column, 4096.0), axis=1, keepdims=True)
    second = jnp.max(jnp.where(plus, column, -1.0), axis=1, keepdims=True)
    long = jnp.sum(jnp.where(value == -1, column, 0.0), axis=1, keepdims=True)
    lane = lax.broadcasted_iota(jnp.int32, (inc.shape[0], LANES), 1)
    three = jnp.where(lane == 0, first, jnp.where(lane == 1, second, long))
    spot = 16 * lax.rem(me, 8)
    rest16[pl.ds(pl.multiple_of(spot, 16), 16), :] = three[LANES:]
    here = lax.broadcasted_iota(jnp.int32, (8, LANES), 1) // 16 == lax.rem(me, 8)
    for q, t, w in (
        (0, three[:LANES], wrow[:, :LANES]),
        (1, rest16[...], pltpu.roll(wrow[:, LANES:], spot, 1)),
    ):
        t = jnp.transpose(t)[0:8]
        block = jnp.floor((t + 0.5) * (1.0 / rows))
        high = w[0:1].astype(jnp.bfloat16).astype(jnp.float32)
        message = jnp.concatenate([(t - block * rows)[0:3], block[0:3], high, w[0:1] - high], axis=0)
        idx[:, q * LANES : (q + 1) * LANES] = jnp.where(jnp.logical_or(q == 0, here), message, 0.0).astype(jnp.bfloat16)

    pl.semaphore_wait(barrier, GROUP + 4)
    tell_along_z(near1, 1)

    def put(src, dst, send, recv, device):
        @pl.when(device != me)
        def _():
            pltpu.make_async_remote_copy(
                src_ref=src, dst_ref=dst, send_sem=send, recv_sem=recv,
                device_id={"ifg": device}, device_id_type=pl.DeviceIdType.MESH,
            ).start()

        @pl.when(device == me)
        def _():
            pltpu.make_async_copy(src, dst, recv).start()

    def took(ref, sem):
        pltpu.make_async_copy(ref, ref, sem).wait()

    def to_shares(body):
        @pl.loop(0, GROUP)
        def _(j):
            device = peer(j)
            their = rank_of(device, core)

            @pl.when(their < 3)
            def _():
                body(device, pl.multiple_of((3 * (device // 4) + their) * LANES, LANES))

    to_shares(lambda d, at: put(idx, idxs.at[me], idx_s, idx_r.at[me // 2], d))
    to_shares(lambda d, at: put(padded.at[:, pl.ds(at, LANES)], ph.at[me], ph_s, ph_r.at[me // 8], d))

    pl.semaphore_wait(near1, 2)
    tell_along_z(near2, 2)
    pl.semaphore_wait(near2, 2)
    tell_along_z(near4, 4)

    def pair(j):
        return lax.rem(me // 2 + j, GROUP // 2)

    def build(j):
        t = tiles[j]
        at = iota[...]
        lines = []
        blocks = []
        for i in range(3):
            row = jnp.broadcast_to(t[i : i + 1], at.shape).astype(jnp.bfloat16)
            lines.append(jnp.where(at == row, jnp.full_like(at, -1.0 if i == 2 else 1.0), jnp.zeros_like(at)))
            blocks.append(jnp.broadcast_to(t[3 + i : 4 + i], (16, at.shape[1])).astype(jnp.bfloat16))
        one = jnp.ones_like(blocks[0])
        for b in range(GROUP):
            inside = [jnp.where(v == one * b, one, jnp.zeros_like(one)) for v in blocks]
            for g in range(depth // 16):
                terms = [v * line[16 * g : 16 * g + 16] for v, line in zip(inside, lines)]
                inct[j, b * depth + 16 * g : b * depth + 16 * g + 16, :] = terms[0] + terms[1] + terms[2]

    def weights(j):
        return tiles[j, 6:7, :] + tiles[j, 7:8, :]

    def finish(j, count):
        lost = acc[...]
        for q in range(count):
            sine, loss = sin_and_twice_loss(clo[q])
            lost = lost + loss * (0.5 * weights(j + q))
            wb[j + q] = jnp.transpose(sine).astype(jnp.bfloat16)
        acc[...] = lost

    def send_pair(j):
        for q in range(2):
            d = 2 * pair(j) + q
            put(wb.at[j, pl.ds(q * LANES, LANES)], res_ref.at[pl.ds(0, LANES), my_lanes], res_s, res_r, d)

    @pl.when(active)
    def _():
        @pl.loop(0, GROUP // 2)
        def _(j):
            p = pair(j)
            took(idxs.at[pl.ds(2 * p, 2)], idx_r.at[p])
            for q in range(2):
                tiles[j, :, q * LANES : (q + 1) * LANES] = idxs[2 * p + q, :, 0:LANES].astype(jnp.float32)
            build(j)

        for q in range(2):
            rest = idxs[8 * q, :, LANES:].astype(jnp.float32)
            for i in range(1, 8):
                rest = rest + idxs[8 * q + i, :, LANES:].astype(jnp.float32)
            tiles[GROUP // 2, :, q * LANES : (q + 1) * LANES] = rest

        build(steps - 1)

        for half in range(2):
            took(ph.at[pl.ds(8 * half, 8)], ph_r.at[half])
            block = ph[8 * half : 8 * half + 8].reshape(8 * depth, LANES)
            pht[:, 8 * depth * half : 8 * depth * (half + 1)] = jnp.transpose(block.astype(jnp.float32)).astype(jnp.bfloat16)

        def multiply(j):
            return jnp.dot(pht[...], inct[j], preferred_element_type=jnp.float32)

        for q in range(2):
            clo[q] = multiply(q)

        @pl.loop(1, GROUP // 4)
        def _(g):
            closure = [multiply(2 * g + q) for q in range(2)]
            finish(2 * g - 2, 2)
            for q in range(2):
                clo[q] = closure[q]
            for q in range(2):
                send_pair(2 * g - 2 + q)

        closure = multiply(steps - 1)
        finish(steps - 3, 2)
        clo[0] = closure
        for q in range(2):
            send_pair(steps - 3 + q)
        finish(steps - 1, 1)

        total = weights(0)
        for j in range(1, steps):
            total = total + weights(j)
        both = acc[:, 0:LANES] + acc[:, LANES:]
        misfit = jnp.sum(jnp.transpose(both), axis=0, keepdims=True)
        scores[pix] = misfit / jnp.sum(total, axis=1, keepdims=True)

    pl.semaphore_wait(near4, 2)

    @pl.loop(0, pixes - 1)
    def _(k):
        other = far(k)
        pltpu.make_async_remote_copy(
            src_ref=scores.at[pix], dst_ref=scores.at[pix], send_sem=pix_s, recv_sem=pix_r,
            device_id={"pix": other}, device_id_type=pl.DeviceIdType.MESH,
        ).start()

    @pl.when(active)
    def _():
        @pl.loop(0, GROUP)
        def _(k):
            d = peer(k)
            put(
                wb.at[steps - 1, pl.ds(pl.multiple_of(16 * d, 16), 16)],
                res_ref.at[pl.ds(LANES, 16), my_lanes], lef_s, res_r, d,
            )

        @pl.loop(0, 4)
        def _(j):
            c = lax.rem(x + 2 + j, 4)
            at = pl.ds(pl.multiple_of(c * 4 * depth, 4 * depth), 4 * depth)
            corr = jnp.zeros((4 * depth, LANES), jnp.float32)
            for p in range(steps):
                corr = corr + jnp.dot(inct[p, at, :], wb[p], preferred_element_type=jnp.float32)
            cb[pl.ds(4 * c, 4)] = corr.astype(jnp.bfloat16).reshape(4, depth, LANES)
            for q in range(4):
                d = 4 * c + q
                put(cb.at[d], cor_ref.at[:, my_lanes], cor_s, cor_r, d)

    took(scores.at[pl.ds(0, pixes - 1)], pix_r)

    fin_out[0:1] = scores[pix]
    fin_out[1:2] = jnp.sum(scores[...], axis=0)
    slot = jnp.where(active, share, 12 + x)

    @pl.loop(0, GROUP)
    def _(k):
        d = peer(k)
        put(fin_out, fin.at[slot], fin_s, fin_r, d)

    others = GROUP - 1
    took(scores.at[pl.ds(0, pixes - 1)], pix_s)

    @pl.when(active)
    def _():
        took(idxs.at[pl.ds(0, 11)], idx_s)
        took(ph.at[pl.ds(0, 11)], ph_s)
        took(inct.at[0, pl.ds(0, others * LANES // 2)], res_s)
        took(wb.at[0, pl.ds(0, others * 16)], lef_s)
        took(cb.at[pl.ds(0, others)], cor_s)

    @pl.when(rank == 3)
    def _():
        took(idxs.at[pl.ds(0, 12)], idx_s)
        took(ph.at[pl.ds(0, 12)], ph_s)

    took(res_ref, res_r)
    took(cor_ref, cor_r)

    span = (dates[1:2] - dates[0:1]).astype(jnp.float32)
    damp = jnp.concatenate([1.0 / (2.0 + span), jnp.zeros((1, LANES - rows), jnp.float32)], axis=1)
    damp = jnp.transpose(jnp.broadcast_to(damp, (LANES, LANES)))[:rows]

    @pl.loop(0, 12)
    def _(s):
        lanes = pl.ds(pl.multiple_of(s * LANES, LANES), LANES)
        residual_ref[:, lanes] = res_ref[:, lanes].astype(jnp.float32)
        corrected_ref[:, lanes] = phase[:, lanes].astype(jnp.float32) - cor_ref[0:rows, lanes].astype(jnp.float32) * damp

    took(fin.at[pl.ds(0, others)], fin_s)
    took(fin, fin_r)

    everything = jnp.sum(jnp.sum(fin[...], axis=0)[1:2], axis=1, keepdims=True)
    for s in range(12):
        rel_ref[:, s * LANES : (s + 1) * LANES] = fin[s, 0:1] / (everything / all_pixels)


def store(*refs):
    n = len(refs) // 2
    sems = refs[-1]
    flat = [r.at[0] if r.shape[0] == 1 else r for r in refs[:n]]
    copies = [pltpu.make_async_copy(flat[i], refs[n + i], sems.at[i]) for i in range(n)]
    for copy in copies:
        copy.start()
    for copy in copies:
        copy.wait()


def local(phase, incidence, triplet_weight, date_pairs):
    rows, pixel_count = phase.shape
    depth = -(-rows // 16) * 16
    triplets = incidence.shape[0]
    pairs = GROUP // 2 + 1
    hbm = pl.BlockSpec(memory_space=pltpu.HBM)
    vmem = pl.BlockSpec(memory_space=pltpu.VMEM)
    pixes = lax.axis_size("pix")
    operands = (phase, incidence, triplet_weight.reshape(1, triplets), date_pairs.T)
    operands = [pltpu.with_memory_space_constraint(a, pltpu.HBM) for a in operands]
    residual, relative, corrected = pl.pallas_call(
        functools.partial(kernel, pixes * pixel_count),
        out_shape=(
            jax.ShapeDtypeStruct((triplets, pixel_count), jnp.float32),
            jax.ShapeDtypeStruct((1, pixel_count), jnp.float32),
            jax.ShapeDtypeStruct((rows, pixel_count), jnp.float32),
        ),
        in_specs=[hbm] * 4,
        out_specs=[vmem] * 3,
        scratch_shapes=[
            pltpu.VMEM(incidence.shape, jnp.int32),
            pltpu.VMEM(phase.shape, jnp.bfloat16),
            pltpu.VMEM((1, triplets), jnp.float32),
            pltpu.VMEM((2, rows), jnp.int32),
            pltpu.VMEM((triplets, pixel_count), jnp.bfloat16),
            pltpu.VMEM((depth, pixel_count), jnp.bfloat16),
            pltpu.VMEM((8, 2 * LANES), jnp.bfloat16),
            pltpu.VMEM((LANES, LANES), jnp.float32),
            pltpu.VMEM((8, 2 * LANES), jnp.float32),
            pltpu.VMEM((depth, pixel_count), jnp.bfloat16),
            pltpu.VMEM((GROUP, depth, LANES), jnp.bfloat16),
            pltpu.VMEM((LANES, GROUP * depth), jnp.bfloat16),
            pltpu.VMEM((GROUP, 8, 2 * LANES), jnp.bfloat16),
            pltpu.VMEM((pairs, 8, 2 * LANES), jnp.float32),
            pltpu.VMEM((pairs, GROUP * depth, 2 * LANES), jnp.bfloat16),
            pltpu.VMEM((depth, 2 * LANES), jnp.bfloat16),
            pltpu.VMEM((2, LANES, 2 * LANES), jnp.float32),
            pltpu.VMEM((pairs, 2 * LANES, LANES), jnp.bfloat16),
            pltpu.VMEM((GROUP, depth, LANES), jnp.bfloat16),
            pltpu.VMEM((LANES, 2 * LANES), jnp.float32),
            pltpu.VMEM((pixes, 1, LANES), jnp.float32),
            pltpu.VMEM((2, LANES), jnp.float32),
            pltpu.VMEM((GROUP, 2, LANES), jnp.float32),
            pltpu.SemaphoreType.DMA((4,)),
            pltpu.SemaphoreType.DMA((2,)),
            pltpu.SemaphoreType.DMA((GROUP // 2,)),
            *[pltpu.SemaphoreType.DMA] * 11,
            *[pltpu.SemaphoreType.REGULAR] * 3,
        ],
        compiler_params=pltpu.CompilerParams(collective_id=0, has_side_effects=True, vmem_limit_bytes=VMEM),
    )(*operands)
    return pl.pallas_call(
        store,
        out_shape=(
            jax.ShapeDtypeStruct(residual.shape, jnp.float32),
            jax.ShapeDtypeStruct((pixel_count,), jnp.float32),
            jax.ShapeDtypeStruct(corrected.shape, jnp.float32),
        ),
        in_specs=[pl.BlockSpec(memory_space=pl.ANY)] * 3,
        out_specs=[hbm] * 3,
        scratch_shapes=[pltpu.SemaphoreType.DMA((3,))],
        compiler_params=pltpu.CompilerParams(vmem_limit_bytes=1024 * 1024),
    )(residual, relative, corrected)


def solution(mesh):
    return jax.shard_map(
        local,
        mesh=mesh,
        in_specs=(P("ifg", "pix"), P("ifg", None), P("ifg"), P("ifg", None)),
        out_specs=(P("ifg", "pix"), P("pix"), P("ifg", "pix")),
        check_vma=False,
    )
```

```python
import functools

import jax
import jax.numpy as jnp
from jax import lax
from jax.experimental import pallas as pl
from jax.experimental.pallas import tpu as pltpu
from jax.sharding import PartitionSpec as P

GROUP = 16
LANES = 128
EARLY = 2
VMEM = 16 * 1024 * 1024
INV_2PI = 0.15915494309189535
TWO_PI_HI = 6.28125
TWO_PI_LO = 1.9353071795864769e-3
SIN = (-0.041666642741103474, 0.000520813580633296, -3.094783609930149e-06, 1.0156463124188801e-08)
COS = (-0.12499999887388552, 0.0026041650454957602, -2.170063047895746e-05, 9.672611781418933e-08, -2.5465921654786513e-10)


def poly(coefs, z):
    out = z * coefs[-1] + coefs[-2]
    for c in coefs[-3::-1]:
        out = out * z + c
    return out


def sin_and_twice_loss(x):
    k = jnp.round(x * INV_2PI)
    r = (x - k * TWO_PI_HI) - k * TWO_PI_LO
    z = r * r
    sine = r + (r * z) * poly(SIN, z)
    cosine = 1.0 + z * poly(COS, z)
    return sine * cosine, sine * sine


PEERS = sorted(
    ((dx, dy) for dx in range(4) for dy in range(4) if dx or dy),
    key=lambda p: -min(p[0], 4 - p[0]) - min(p[1], 4 - p[1]),
)


def rank_of(device, core):
    return lax.rem(lax.rem(device, 4) + device // 4 + 2 * core, 4)


def kernel(
    all_pixels,
    phase_hbm, inc_hbm, weight_hbm, dates_hbm, residual_ref, rel_ref, corrected_ref,
    inc, phase, weight, dates, res_ref, cor_ref, idx, rest16, wrow, padded, ph, pht, idxs, tiles, inct, iota, clo, wb, cb, acc, scores, fin_out, fin,
    in_sem, ph_r, idx_r, idx_s, ph_s, res_s, res_r, lef_s, cor_s, cor_r, fin_s, fin_r, pix_s, pix_r,
    near1, near2, near4,
):
    me = lax.axis_index("ifg")
    pix = lax.axis_index("pix")
    x, y = me // 4, lax.rem(me, 4)
    core = lax.rem(pix, 2)
    rank = rank_of(me, core)
    active = rank < 3
    share = 3 * x + rank
    my_lanes = pl.ds(pl.multiple_of(share * LANES, LANES), LANES)
    rows = phase.shape[0]
    depth = padded.shape[0]
    pixes = scores.shape[0]
    steps = GROUP // 2 + 1

    def peer(dx, dy):
        return xs[dx] + ys[dy]

    xs = [4 * lax.rem(x + i, 4) for i in range(4)]
    ys = [lax.rem(y + i, 4) for i in range(4)]

    def far(k):
        return lax.rem(pix + pixes // 2 + (k + 1) // 2 * (1 - 2 * (k % 2)), pixes)

    barrier = pltpu.get_barrier_semaphore()

    def tell_group(k):
        pl.semaphore_signal(barrier, inc=1, device_id={"ifg": lax.rem(me + k, GROUP)}, device_id_type=pl.DeviceIdType.MESH)

    def tell_pix(sem, other):
        pl.semaphore_signal(sem, inc=1, device_id={"pix": lax.rem(other, pixes)}, device_id_type=pl.DeviceIdType.MESH)

    def tell_along_z(sem, distance):
        tell_pix(sem, pix + 2 * distance)
        tell_pix(sem, pix + pixes - 2 * distance)

    read_inc = pltpu.make_async_copy(inc_hbm, inc, in_sem.at[0])
    read_inc.start()
    read_phase = pltpu.make_async_copy(phase_hbm, phase, in_sem.at[1])
    read_phase.start()
    read_weight = pltpu.make_async_copy(weight_hbm, weight, in_sem.at[2])
    read_weight.start()
    read_dates = pltpu.make_async_copy(dates_hbm, dates, in_sem.at[3])
    read_dates.start()
    pl.loop(1, GROUP)(tell_group)
    across = 2 * (pix // 2) + 1 - core
    tell_pix(barrier, across)
    tell_along_z(barrier, 1)
    tell_pix(barrier, across + 2)
    tell_pix(barrier, across + pixes - 2)

    iota[...] = lax.broadcasted_iota(jnp.int32, iota.shape, 0).astype(jnp.float32).astype(jnp.bfloat16)
    acc[...] = jnp.zeros_like(acc)
    scores[pix] = jnp.zeros(scores.shape[1:], scores.dtype)
    wrow[...] = jnp.zeros_like(wrow)
    rest16[...] = jnp.zeros_like(rest16)
    padded[...] = jnp.zeros_like(padded)

    read_inc.wait()
    read_phase.wait()
    read_weight.wait()
    read_dates.wait()
    padded[0:rows, :] = phase[...]
    wrow[0:1, 0 : weight.shape[1]] = weight[...]
    width = inc.shape[1]
    column = lax.broadcasted_iota(jnp.int32, (1, width), 1).astype(jnp.float32)
    value = inc[...]
    plus = value == 1
    first = jnp.min(jnp.where(plus, column, 4096.0), axis=1, keepdims=True)
    second = jnp.max(jnp.where(plus, column, -1.0), axis=1, keepdims=True)
    long = jnp.sum(jnp.where(value == -1, column, 0.0), axis=1, keepdims=True)
    lane = lax.broadcasted_iota(jnp.int32, (inc.shape[0], LANES), 1)
    three = jnp.where(lane == 0, first, jnp.where(lane == 1, second, long))
    spot = 16 * lax.rem(me, 8)
    rest16[pl.ds(pl.multiple_of(spot, 16), 16), :] = three[LANES:]
    here = lax.broadcasted_iota(jnp.int32, (8, LANES), 1) // 16 == lax.rem(me, 8)
    for q, t, w in (
        (0, three[:LANES], wrow[:, :LANES]),
        (1, rest16[...], pltpu.roll(wrow[:, LANES:], spot, 1)),
    ):
        t = jnp.transpose(t)[0:8]
        block = jnp.floor((t + 0.5) * (1.0 / rows))
        high = w[0:1].astype(jnp.bfloat16).astype(jnp.float32)
        message = jnp.concatenate([(t - block * rows)[0:3], block[0:3], high, w[0:1] - high], axis=0)
        idx[:, q * LANES : (q + 1) * LANES] = jnp.where(jnp.logical_or(q == 0, here), message, 0.0).astype(jnp.bfloat16)

    pl.semaphore_wait(barrier, GROUP + 4)
    tell_along_z(near1, 1)

    def put(src, dst, send, recv, device):
        pltpu.make_async_remote_copy(
            src_ref=src, dst_ref=dst, send_sem=send, recv_sem=recv,
            device_id={"ifg": device}, device_id_type=pl.DeviceIdType.MESH,
        ).start()

    def keep(src, dst, recv):
        pltpu.make_async_copy(src, dst, recv).start()

    def took(ref, sem):
        pltpu.make_async_copy(ref, ref, sem).wait()

    def to_shares(body, own):
        for e in (0, 1, 3, 2):
            their = lax.rem(x + y + 2 * core + e, 4)

            @pl.when(their < 3)
            def _():
                for dx, dy in PEERS:
                    if (dx + dy) % 4 == e:
                        at = pl.multiple_of((3 * lax.rem(x + dx, 4) + their) * LANES, LANES)
                        body(peer(dx, dy), at)
                if e == 0:
                    own()

    here_idx = idx_r.at[me // 2]
    here_ph = ph_r.at[me // 8]
    to_shares(lambda d, at: put(idx, idxs.at[me], idx_s, here_idx, d), lambda: keep(idx, idxs.at[me], here_idx))
    pl.semaphore_wait(near1, 2)
    tell_along_z(near2, 2)
    to_shares(
        lambda d, at: put(padded.at[:, pl.ds(at, LANES)], ph.at[me], ph_s, here_ph, d),
        lambda: keep(padded.at[:, my_lanes], ph.at[me], here_ph),
    )

    def pair(j):
        return lax.rem(me // 2 + 1 + j, GROUP // 2)

    def build(j):
        t = tiles[j]
        at = iota[...]
        lines = []
        blocks = []
        for i in range(3):
            row = jnp.broadcast_to(t[i : i + 1], at.shape).astype(jnp.bfloat16)
            lines.append(jnp.where(at == row, jnp.full_like(at, -1.0 if i == 2 else 1.0), jnp.zeros_like(at)))
            blocks.append(jnp.broadcast_to(t[3 + i : 4 + i], (16, at.shape[1])).astype(jnp.bfloat16))
        one = jnp.ones_like(blocks[0])
        for b in range(GROUP):
            inside = [jnp.where(v == one * b, one, jnp.zeros_like(one)) for v in blocks]
            for g in range(depth // 16):
                terms = [v * line[16 * g : 16 * g + 16] for v, line in zip(inside, lines)]
                inct[j, b * depth + 16 * g : b * depth + 16 * g + 16, :] = terms[0] + terms[1] + terms[2]

    def weights(j):
        return tiles[j, 6:7, :] + tiles[j, 7:8, :]

    def finish(j, count):
        lost = acc[...]
        for q in range(count):
            sine, loss = sin_and_twice_loss(clo[q])
            lost = lost + loss * (0.5 * weights(j + q))
            wb[j + q] = jnp.transpose(sine).astype(jnp.bfloat16)
        acc[...] = lost

    mine = res_ref.at[pl.ds(0, LANES), my_lanes]
    mine16 = res_ref.at[pl.ds(LANES, 16), my_lanes]

    def send_pair(j):
        for q in range(2):
            put(wb.at[j, pl.ds(q * LANES, LANES)], mine, res_s, res_r, 2 * pair(j) + q)

    def send_own_pair(j):
        odd = lax.rem(me, 2)
        own = pl.ds(pl.multiple_of(odd * LANES, LANES), LANES)
        next_door = pl.ds(pl.multiple_of((1 - odd) * LANES, LANES), LANES)
        put(wb.at[j, next_door], mine, res_s, res_r, me + 1 - 2 * odd)
        keep(wb.at[j, own], mine, res_r)

    @pl.when(rank == 3)
    def _():
        pl.semaphore_wait(near2, 2)
        tell_along_z(near4, 4)

    @pl.when(active)
    def _():
        def arrived(j):
            p = pair(j)
            took(idxs.at[pl.ds(2 * p, 2)], idx_r.at[p])
            for q in range(2):
                tiles[j, :, q * LANES : (q + 1) * LANES] = idxs[2 * p + q, :, 0:LANES].astype(jnp.float32)
            build(j)

        pl.loop(0, EARLY)(arrived)
        pl.semaphore_wait(near2, 2)
        tell_along_z(near4, 4)
        pl.loop(EARLY, GROUP // 2)(arrived)

        for q in range(2):
            rest = idxs[8 * q, :, LANES:].astype(jnp.float32)
            for i in range(1, 8):
                rest = rest + idxs[8 * q + i, :, LANES:].astype(jnp.float32)
            tiles[GROUP // 2, :, q * LANES : (q + 1) * LANES] = rest

        build(steps - 1)

        for half in range(2):
            took(ph.at[pl.ds(8 * half, 8)], ph_r.at[half])
            block = ph[8 * half : 8 * half + 8].reshape(8 * depth, LANES)
            pht[:, 8 * depth * half : 8 * depth * (half + 1)] = jnp.transpose(block.astype(jnp.float32)).astype(jnp.bfloat16)

        def multiply(j):
            return jnp.dot(pht[...], inct[j], preferred_element_type=jnp.float32)

        for q in range(2):
            clo[q] = multiply(q)

        @pl.loop(1, GROUP // 4)
        def _(g):
            closure = [multiply(2 * g + q) for q in range(2)]
            finish(2 * g - 2, 2)
            for q in range(2):
                clo[q] = closure[q]
            for q in range(2):
                send_pair(2 * g - 2 + q)

        closure = multiply(steps - 1)
        finish(steps - 3, 2)
        clo[0] = closure
        send_pair(steps - 3)
        send_own_pair(steps - 2)
        finish(steps - 1, 1)

        total = weights(0)
        for j in range(1, steps):
            total = total + weights(j)
        both = acc[:, 0:LANES] + acc[:, LANES:]
        misfit = jnp.sum(jnp.transpose(both), axis=0, keepdims=True)
        scores[pix] = misfit / jnp.sum(total, axis=1, keepdims=True)

    pl.semaphore_wait(near4, 2)

    for k in range(pixes - 1):
        pltpu.make_async_remote_copy(
            src_ref=scores.at[pix], dst_ref=scores.at[pix], send_sem=pix_s, recv_sem=pix_r,
            device_id={"pix": far(k)}, device_id_type=pl.DeviceIdType.MESH,
        ).start()

    @pl.when(active)
    def _():
        def sixteen(d):
            return wb.at[steps - 1, pl.ds(pl.multiple_of(16 * d, 16), 16)]

        for dx, dy in PEERS:
            put(sixteen(peer(dx, dy)), mine16, lef_s, res_r, peer(dx, dy))
        keep(sixteen(me), mine16, res_r)

        @pl.loop(0, 4)
        def _(j):
            c = lax.rem(x + 2 + j, 4)
            at = pl.ds(pl.multiple_of(c * 4 * depth, 4 * depth), 4 * depth)
            corr = jnp.zeros((4 * depth, LANES), jnp.float32)
            for p in range(steps):
                corr = corr + jnp.dot(inct[p, at, :], wb[p], preferred_element_type=jnp.float32)
            cb[pl.ds(4 * c, 4)] = corr.astype(jnp.bfloat16).reshape(4, depth, LANES)
            for q in range(4):
                d = 4 * c + q

                @pl.when(d != me)
                def _():
                    put(cb.at[d], cor_ref.at[:, my_lanes], cor_s, cor_r, d)

                @pl.when(d == me)
                def _():
                    keep(cb.at[d], cor_ref.at[:, my_lanes], cor_r)

    took(scores.at[pl.ds(0, pixes - 1)], pix_r)

    fin_out[0:1] = scores[pix]
    fin_out[1:2] = jnp.sum(scores[...], axis=0)
    slot = jnp.where(active, share, 12 + x)

    for dx, dy in PEERS:
        put(fin_out, fin.at[slot], fin_s, fin_r, peer(dx, dy))
    keep(fin_out, fin.at[slot], fin_r)

    others = GROUP - 1
    took(scores.at[pl.ds(0, pixes - 1)], pix_s)

    @pl.when(active)
    def _():
        took(idxs.at[pl.ds(0, 11)], idx_s)
        took(ph.at[pl.ds(0, 11)], ph_s)
        took(inct.at[0, pl.ds(0, others * LANES // 2)], res_s)
        took(wb.at[0, pl.ds(0, others * 16)], lef_s)
        took(cb.at[pl.ds(0, others)], cor_s)

    @pl.when(rank == 3)
    def _():
        took(idxs.at[pl.ds(0, 12)], idx_s)
        took(ph.at[pl.ds(0, 12)], ph_s)

    took(res_ref, res_r)
    took(cor_ref, cor_r)

    span = (dates[1:2] - dates[0:1]).astype(jnp.float32)
    damp = jnp.concatenate([1.0 / (2.0 + span), jnp.zeros((1, LANES - rows), jnp.float32)], axis=1)
    damp = jnp.transpose(jnp.broadcast_to(damp, (LANES, LANES)))[:rows]

    @pl.loop(0, 12)
    def _(s):
        lanes = pl.ds(pl.multiple_of(s * LANES, LANES), LANES)
        residual_ref[:, lanes] = res_ref[:, lanes].astype(jnp.float32)
        corrected_ref[:, lanes] = phase[:, lanes].astype(jnp.float32) - cor_ref[0:rows, lanes].astype(jnp.float32) * damp

    took(fin.at[pl.ds(0, others)], fin_s)
    took(fin, fin_r)

    everything = jnp.sum(jnp.sum(fin[...], axis=0)[1:2], axis=1, keepdims=True)
    for s in range(12):
        rel_ref[:, s * LANES : (s + 1) * LANES] = fin[s, 0:1] / (everything / all_pixels)


def store(residual, relative, corrected, residual_out, relative_out, corrected_out, sems):
    copies = [(relative.at[0], relative_out)]
    for src, dst, step in ((residual, residual_out, 48), (corrected, corrected_out, 40)):
        for at in range(0, src.shape[0], step):
            rows = pl.ds(at, min(step, src.shape[0] - at))
            copies.append((src.at[rows], dst.at[rows]))
    copies = [pltpu.make_async_copy(src, dst, sems.at[i]) for i, (src, dst) in enumerate(copies)]
    for copy in copies:
        copy.start()
    for copy in copies:
        copy.wait()


def local(phase, incidence, triplet_weight, date_pairs):
    rows, pixel_count = phase.shape
    depth = -(-rows // 16) * 16
    triplets = incidence.shape[0]
    pairs = GROUP // 2 + 1
    hbm = pl.BlockSpec(memory_space=pltpu.HBM)
    vmem = pl.BlockSpec(memory_space=pltpu.VMEM)
    pixes = lax.axis_size("pix")
    operands = (phase, incidence, triplet_weight.reshape(1, triplets), date_pairs.T)
    operands = [pltpu.with_memory_space_constraint(a, pltpu.HBM) for a in operands]
    residual, relative, corrected = pl.pallas_call(
        functools.partial(kernel, pixes * pixel_count),
        out_shape=(
            jax.ShapeDtypeStruct((triplets, pixel_count), jnp.float32),
            jax.ShapeDtypeStruct((1, pixel_count), jnp.float32),
            jax.ShapeDtypeStruct((rows, pixel_count), jnp.float32),
        ),
        in_specs=[hbm] * 4,
        out_specs=[vmem] * 3,
        scratch_shapes=[
            pltpu.VMEM(incidence.shape, jnp.int32),
            pltpu.VMEM(phase.shape, jnp.bfloat16),
            pltpu.VMEM((1, triplets), jnp.float32),
            pltpu.VMEM((2, rows), jnp.int32),
            pltpu.VMEM((triplets, pixel_count), jnp.bfloat16),
            pltpu.VMEM((depth, pixel_count), jnp.bfloat16),
            pltpu.VMEM((8, 2 * LANES), jnp.bfloat16),
            pltpu.VMEM((LANES, LANES), jnp.float32),
            pltpu.VMEM((8, 2 * LANES), jnp.float32),
            pltpu.VMEM((depth, pixel_count), jnp.bfloat16),
            pltpu.VMEM((GROUP, depth, LANES), jnp.bfloat16),
            pltpu.VMEM((LANES, GROUP * depth), jnp.bfloat16),
            pltpu.VMEM((GROUP, 8, 2 * LANES), jnp.bfloat16),
            pltpu.VMEM((pairs, 8, 2 * LANES), jnp.float32),
            pltpu.VMEM((pairs, GROUP * depth, 2 * LANES), jnp.bfloat16),
            pltpu.VMEM((depth, 2 * LANES), jnp.bfloat16),
            pltpu.VMEM((2, LANES, 2 * LANES), jnp.float32),
            pltpu.VMEM((pairs, 2 * LANES, LANES), jnp.bfloat16),
            pltpu.VMEM((GROUP, depth, LANES), jnp.bfloat16),
            pltpu.VMEM((LANES, 2 * LANES), jnp.float32),
            pltpu.VMEM((pixes, 1, LANES), jnp.float32),
            pltpu.VMEM((2, LANES), jnp.float32),
            pltpu.VMEM((GROUP, 2, LANES), jnp.float32),
            pltpu.SemaphoreType.DMA((4,)),
            pltpu.SemaphoreType.DMA((2,)),
            pltpu.SemaphoreType.DMA((GROUP // 2,)),
            *[pltpu.SemaphoreType.DMA] * 11,
            *[pltpu.SemaphoreType.REGULAR] * 3,
        ],
        compiler_params=pltpu.CompilerParams(collective_id=0, has_side_effects=True, vmem_limit_bytes=VMEM),
    )(*operands)
    return pl.pallas_call(
        store,
        out_shape=(
            jax.ShapeDtypeStruct(residual.shape, jnp.float32),
            jax.ShapeDtypeStruct((pixel_count,), jnp.float32),
            jax.ShapeDtypeStruct(corrected.shape, jnp.float32),
        ),
        in_specs=[pl.BlockSpec(memory_space=pl.ANY)] * 3,
        out_specs=[hbm] * 3,
        scratch_shapes=[pltpu.SemaphoreType.DMA((6,))],
        compiler_params=pltpu.CompilerParams(vmem_limit_bytes=1024 * 1024),
    )(residual, relative, corrected)


def solution(mesh):
    return jax.shard_map(
        local,
        mesh=mesh,
        in_specs=(P("ifg", "pix"), P("ifg", None), P("ifg"), P("ifg", None)),
        out_specs=(P("ifg", "pix"), P("pix"), P("ifg", "pix")),
        check_vma=False,
    )
```

```python
import functools

import jax
import jax.numpy as jnp
from jax import lax
from jax.experimental import pallas as pl
from jax.experimental.pallas import tpu as pltpu
from jax.sharding import PartitionSpec as P

GROUP = 16
LANES = 128
EARLY = 2
VMEM = 16 * 1024 * 1024
INV_2PI = 0.15915494309189535
TWO_PI_HI = 6.28125
TWO_PI_LO = 1.9353071795864769e-3
SIN = (-0.041666642741103474, 0.000520813580633296, -3.094783609930149e-06, 1.0156463124188801e-08)
COS = (-0.12499999887388552, 0.0026041650454957602, -2.170063047895746e-05, 9.672611781418933e-08, -2.5465921654786513e-10)


def poly(coefs, z):
    out = z * coefs[-1] + coefs[-2]
    for c in coefs[-3::-1]:
        out = out * z + c
    return out


def sin_and_twice_loss(x):
    k = jnp.round(x * INV_2PI)
    r = (x - k * TWO_PI_HI) - k * TWO_PI_LO
    z = r * r
    sine = r + (r * z) * poly(SIN, z)
    cosine = 1.0 + z * poly(COS, z)
    return sine * cosine, sine * sine


PEERS = sorted(
    ((dx, dy) for dx in range(4) for dy in range(4) if dx or dy),
    key=lambda p: -min(p[0], 4 - p[0]) - min(p[1], 4 - p[1]),
)


def rank_of(device, core):
    return lax.rem(lax.rem(device, 4) + device // 4 + 2 * core, 4)


def kernel(
    all_pixels,
    phase_hbm, inc_hbm, weight_hbm, dates_hbm, residual_ref, rel_ref, corrected_ref,
    inc, phase, weight, dates, res_ref, cor_ref, idx, rest16, wrow, padded, ph, pht, idxs, tiles, inct, iota, clo, wb, cb, acc, scores, fin_out, fin,
    in_sem, ph_r, idx_r, idx_s, ph_s, res_s, res_r, lef_s, cor_s, cor_r, fin_s, fin_r, pix_s, pix_r,
    near1, near2, near4,
):
    me = lax.axis_index("ifg")
    pix = lax.axis_index("pix")
    x, y = me // 4, lax.rem(me, 4)
    core = lax.rem(pix, 2)
    rank = rank_of(me, core)
    active = rank < 3
    share = 3 * x + rank
    my_lanes = pl.ds(pl.multiple_of(share * LANES, LANES), LANES)
    rows = phase.shape[0]
    depth = padded.shape[0]
    pixes = scores.shape[0]
    steps = GROUP // 2 + 1

    def peer(dx, dy):
        return xs[dx] + ys[dy]

    xs = [4 * lax.rem(x + i, 4) for i in range(4)]
    ys = [lax.rem(y + i, 4) for i in range(4)]

    def far(k):
        return lax.rem(pix + pixes // 2 + (k + 1) // 2 * (1 - 2 * (k % 2)), pixes)

    barrier = pltpu.get_barrier_semaphore()

    def tell_pix(sem, other):
        pl.semaphore_signal(sem, inc=1, device_id={"pix": lax.rem(other, pixes)}, device_id_type=pl.DeviceIdType.MESH)

    def tell_along_z(sem, distance):
        tell_pix(sem, pix + 2 * distance)
        tell_pix(sem, pix + pixes - 2 * distance)

    for dx, dy in PEERS:
        pl.semaphore_signal(barrier, inc=1, device_id={"ifg": peer(dx, dy)}, device_id_type=pl.DeviceIdType.MESH)
    across = 2 * (pix // 2) + 1 - core
    tell_pix(barrier, across)
    tell_along_z(barrier, 1)
    tell_pix(barrier, across + 2)
    tell_pix(barrier, across + pixes - 2)
    read_inc = pltpu.make_async_copy(inc_hbm, inc, in_sem.at[0])
    read_inc.start()
    read_phase = pltpu.make_async_copy(phase_hbm, phase, in_sem.at[1])
    read_phase.start()
    read_weight = pltpu.make_async_copy(weight_hbm, weight, in_sem.at[2])
    read_weight.start()
    read_dates = pltpu.make_async_copy(dates_hbm, dates, in_sem.at[3])
    read_dates.start()

    iota[...] = lax.broadcasted_iota(jnp.int32, iota.shape, 0).astype(jnp.float32).astype(jnp.bfloat16)
    acc[...] = jnp.zeros_like(acc)
    scores[pix] = jnp.zeros(scores.shape[1:], scores.dtype)
    wrow[...] = jnp.zeros_like(wrow)
    rest16[...] = jnp.zeros_like(rest16)
    padded[...] = jnp.zeros_like(padded)

    read_inc.wait()
    read_phase.wait()
    read_weight.wait()
    read_dates.wait()
    padded[0:rows, :] = phase[...]
    wrow[0:1, 0 : weight.shape[1]] = weight[...]
    width = inc.shape[1]
    column = lax.broadcasted_iota(jnp.int32, (1, width), 1).astype(jnp.float32)
    value = inc[...]
    plus = value == 1
    first = jnp.min(jnp.where(plus, column, 4096.0), axis=1, keepdims=True)
    second = jnp.max(jnp.where(plus, column, -1.0), axis=1, keepdims=True)
    long = jnp.sum(jnp.where(value == -1, column, 0.0), axis=1, keepdims=True)
    lane = lax.broadcasted_iota(jnp.int32, (inc.shape[0], LANES), 1)
    three = jnp.where(lane == 0, first, jnp.where(lane == 1, second, long))
    spot = 16 * lax.rem(me, 8)
    rest16[pl.ds(pl.multiple_of(spot, 16), 16), :] = three[LANES:]
    here = lax.broadcasted_iota(jnp.int32, (8, LANES), 1) // 16 == lax.rem(me, 8)
    for q, t, w in (
        (0, three[:LANES], wrow[:, :LANES]),
        (1, rest16[...], pltpu.roll(wrow[:, LANES:], spot, 1)),
    ):
        t = jnp.transpose(t)[0:8]
        block = jnp.floor((t + 0.5) * (1.0 / rows))
        high = w[0:1].astype(jnp.bfloat16).astype(jnp.float32)
        message = jnp.concatenate([(t - block * rows)[0:3], block[0:3], high, w[0:1] - high], axis=0)
        idx[:, q * LANES : (q + 1) * LANES] = jnp.where(jnp.logical_or(q == 0, here), message, 0.0).astype(jnp.bfloat16)

    pl.semaphore_wait(barrier, GROUP + 4)
    tell_along_z(near1, 1)

    def put(src, dst, send, recv, device):
        pltpu.make_async_remote_copy(
            src_ref=src, dst_ref=dst, send_sem=send, recv_sem=recv,
            device_id={"ifg": device}, device_id_type=pl.DeviceIdType.MESH,
        ).start()

    def keep(src, dst, recv):
        pltpu.make_async_copy(src, dst, recv).start()

    def took(ref, sem):
        pltpu.make_async_copy(ref, ref, sem).wait()

    def to_shares(body, own):
        for e in (0, 1, 3, 2):
            their = lax.rem(x + y + 2 * core + e, 4)

            @pl.when(their < 3)
            def _():
                for dx, dy in PEERS:
                    if (dx + dy) % 4 == e:
                        at = pl.multiple_of((3 * lax.rem(x + dx, 4) + their) * LANES, LANES)
                        body(peer(dx, dy), at)
                if e == 0:
                    own()

    here_idx = idx_r.at[me // 2]
    here_ph = ph_r.at[me // 8]
    to_shares(lambda d, at: put(idx, idxs.at[me], idx_s, here_idx, d), lambda: keep(idx, idxs.at[me], here_idx))
    pl.semaphore_wait(near1, 2)
    tell_along_z(near2, 2)
    to_shares(
        lambda d, at: put(padded.at[:, pl.ds(at, LANES)], ph.at[me], ph_s, here_ph, d),
        lambda: keep(padded.at[:, my_lanes], ph.at[me], here_ph),
    )

    def pair(j):
        return lax.rem(me // 2 + 1 + j, GROUP // 2)

    def build(j):
        t = tiles[j]
        at = iota[...]
        lines = []
        blocks = []
        for i in range(3):
            row = jnp.broadcast_to(t[i : i + 1], at.shape).astype(jnp.bfloat16)
            lines.append(jnp.where(at == row, jnp.full_like(at, -1.0 if i == 2 else 1.0), jnp.zeros_like(at)))
            blocks.append(jnp.broadcast_to(t[3 + i : 4 + i], (16, at.shape[1])).astype(jnp.bfloat16))
        one = jnp.ones_like(blocks[0])
        for b in range(GROUP):
            inside = [jnp.where(v == one * b, one, jnp.zeros_like(one)) for v in blocks]
            for g in range(depth // 16):
                terms = [v * line[16 * g : 16 * g + 16] for v, line in zip(inside, lines)]
                inct[j, b * depth + 16 * g : b * depth + 16 * g + 16, :] = terms[0] + terms[1] + terms[2]

    def weights(j):
        return tiles[j, 6:7, :] + tiles[j, 7:8, :]

    def finish(j, count):
        lost = acc[...]
        for q in range(count):
            sine, loss = sin_and_twice_loss(clo[q])
            lost = lost + loss * (0.5 * weights(j + q))
            wb[j + q] = jnp.transpose(sine).astype(jnp.bfloat16)
        acc[...] = lost

    mine = res_ref.at[pl.ds(0, LANES), my_lanes]
    mine16 = res_ref.at[pl.ds(LANES, 16), my_lanes]

    def send_pair(j):
        for q in range(2):
            put(wb.at[j, pl.ds(q * LANES, LANES)], mine, res_s, res_r, 2 * pair(j) + q)

    def send_own_pair(j):
        odd = lax.rem(me, 2)
        own = pl.ds(pl.multiple_of(odd * LANES, LANES), LANES)
        next_door = pl.ds(pl.multiple_of((1 - odd) * LANES, LANES), LANES)
        put(wb.at[j, next_door], mine, res_s, res_r, me + 1 - 2 * odd)
        keep(wb.at[j, own], mine, res_r)

    @pl.when(rank == 3)
    def _():
        pl.semaphore_wait(near2, 2)
        tell_along_z(near4, 4)

    @pl.when(active)
    def _():
        def arrived(k):
            p = lax.rem(k + 1, GROUP // 2)
            j = lax.rem(p - me // 2 + GROUP // 2 - 1, GROUP // 2)
            took(idxs.at[pl.ds(2 * p, 2)], idx_r.at[p])
            for q in range(2):
                tiles[j, :, q * LANES : (q + 1) * LANES] = idxs[2 * p + q, :, 0:LANES].astype(jnp.float32)
            build(j)

        pl.loop(0, EARLY)(arrived)
        pl.semaphore_wait(near2, 2)
        tell_along_z(near4, 4)
        pl.loop(EARLY, GROUP // 2)(arrived)

        for q in range(2):
            rest = idxs[8 * q, :, LANES:].astype(jnp.float32)
            for i in range(1, 8):
                rest = rest + idxs[8 * q + i, :, LANES:].astype(jnp.float32)
            tiles[GROUP // 2, :, q * LANES : (q + 1) * LANES] = rest

        build(steps - 1)

        for half in range(2):
            took(ph.at[pl.ds(8 * half, 8)], ph_r.at[half])
            block = ph[8 * half : 8 * half + 8].reshape(8 * depth, LANES)
            pht[:, 8 * depth * half : 8 * depth * (half + 1)] = jnp.transpose(block.astype(jnp.float32)).astype(jnp.bfloat16)

        def multiply(j):
            return jnp.dot(pht[...], inct[j], preferred_element_type=jnp.float32)

        for q in range(2):
            clo[q] = multiply(q)

        @pl.loop(1, GROUP // 4)
        def _(g):
            closure = [multiply(2 * g + q) for q in range(2)]
            finish(2 * g - 2, 2)
            for q in range(2):
                clo[q] = closure[q]
            for q in range(2):
                send_pair(2 * g - 2 + q)

        closure = multiply(steps - 1)
        finish(steps - 3, 2)
        clo[0] = closure
        finish(steps - 1, 1)

        total = weights(0)
        for j in range(1, steps):
            total = total + weights(j)
        both = acc[:, 0:LANES] + acc[:, LANES:]
        misfit = jnp.sum(jnp.transpose(both), axis=0, keepdims=True)
        scores[pix] = misfit / jnp.sum(total, axis=1, keepdims=True)

    pl.semaphore_wait(near4, 2)

    for k in range(pixes - 1):
        pltpu.make_async_remote_copy(
            src_ref=scores.at[pix], dst_ref=scores.at[pix], send_sem=pix_s, recv_sem=pix_r,
            device_id={"pix": far(k)}, device_id_type=pl.DeviceIdType.MESH,
        ).start()

    @pl.when(active)
    def _():
        send_pair(steps - 3)
        send_own_pair(steps - 2)

        def sixteen(d):
            return wb.at[steps - 1, pl.ds(pl.multiple_of(16 * d, 16), 16)]

        for dx, dy in PEERS:
            put(sixteen(peer(dx, dy)), mine16, lef_s, res_r, peer(dx, dy))
        keep(sixteen(me), mine16, res_r)

        @pl.loop(0, 4)
        def _(j):
            c = lax.rem(x + 2 + j, 4)
            at = pl.ds(pl.multiple_of(c * 4 * depth, 4 * depth), 4 * depth)
            corr = jnp.zeros((4 * depth, LANES), jnp.float32)
            for p in range(steps):
                corr = corr + jnp.dot(inct[p, at, :], wb[p], preferred_element_type=jnp.float32)
            cb[pl.ds(4 * c, 4)] = corr.astype(jnp.bfloat16).reshape(4, depth, LANES)
            for q in range(4):
                d = 4 * c + q

                @pl.when(d != me)
                def _():
                    put(cb.at[d], cor_ref.at[:, my_lanes], cor_s, cor_r, d)

                @pl.when(d == me)
                def _():
                    keep(cb.at[d], cor_ref.at[:, my_lanes], cor_r)

    took(scores.at[pl.ds(0, pixes - 1)], pix_r)

    fin_out[0:1] = scores[pix]
    fin_out[1:2] = jnp.sum(scores[...], axis=0)
    slot = jnp.where(active, share, 12 + x)

    for dx, dy in PEERS:
        put(fin_out, fin.at[slot], fin_s, fin_r, peer(dx, dy))
    keep(fin_out, fin.at[slot], fin_r)

    others = GROUP - 1
    took(scores.at[pl.ds(0, pixes - 1)], pix_s)

    @pl.when(active)
    def _():
        took(idxs.at[pl.ds(0, 11)], idx_s)
        took(ph.at[pl.ds(0, 11)], ph_s)
        took(inct.at[0, pl.ds(0, others * LANES // 2)], res_s)
        took(wb.at[0, pl.ds(0, others * 16)], lef_s)
        took(cb.at[pl.ds(0, others)], cor_s)

    @pl.when(rank == 3)
    def _():
        took(idxs.at[pl.ds(0, 12)], idx_s)
        took(ph.at[pl.ds(0, 12)], ph_s)

    took(res_ref, res_r)
    took(cor_ref, cor_r)

    span = (dates[1:2] - dates[0:1]).astype(jnp.float32)
    damp = jnp.concatenate([1.0 / (2.0 + span), jnp.zeros((1, LANES - rows), jnp.float32)], axis=1)
    damp = jnp.transpose(jnp.broadcast_to(damp, (LANES, LANES)))[:rows]

    @pl.loop(0, 12)
    def _(s):
        lanes = pl.ds(pl.multiple_of(s * LANES, LANES), LANES)
        residual_ref[:, lanes] = res_ref[:, lanes].astype(jnp.float32)
        corrected_ref[:, lanes] = phase[:, lanes].astype(jnp.float32) - cor_ref[0:rows, lanes].astype(jnp.float32) * damp

    took(fin.at[pl.ds(0, others)], fin_s)
    took(fin, fin_r)

    everything = jnp.sum(jnp.sum(fin[...], axis=0)[1:2], axis=1, keepdims=True)
    for s in range(12):
        rel_ref[:, s * LANES : (s + 1) * LANES] = fin[s, 0:1] / (everything / all_pixels)


def store(residual, relative, corrected, residual_out, relative_out, corrected_out, sems):
    copies = [(relative.at[0], relative_out)]
    for src, dst, step in ((residual, residual_out, 48), (corrected, corrected_out, 40)):
        for at in range(0, src.shape[0], step):
            rows = pl.ds(at, min(step, src.shape[0] - at))
            copies.append((src.at[rows], dst.at[rows]))
    copies = [pltpu.make_async_copy(src, dst, sems.at[i]) for i, (src, dst) in enumerate(copies)]
    for copy in copies:
        copy.start()
    for copy in copies:
        copy.wait()


def local(phase, incidence, triplet_weight, date_pairs):
    rows, pixel_count = phase.shape
    depth = -(-rows // 16) * 16
    triplets = incidence.shape[0]
    pairs = GROUP // 2 + 1
    hbm = pl.BlockSpec(memory_space=pltpu.HBM)
    vmem = pl.BlockSpec(memory_space=pltpu.VMEM)
    pixes = lax.axis_size("pix")
    operands = (phase, incidence, triplet_weight.reshape(1, triplets), date_pairs.T)
    operands = [pltpu.with_memory_space_constraint(a, pltpu.HBM) for a in operands]
    residual, relative, corrected = pl.pallas_call(
        functools.partial(kernel, pixes * pixel_count),
        out_shape=(
            jax.ShapeDtypeStruct((triplets, pixel_count), jnp.float32),
            jax.ShapeDtypeStruct((1, pixel_count), jnp.float32),
            jax.ShapeDtypeStruct((rows, pixel_count), jnp.float32),
        ),
        in_specs=[hbm] * 4,
        out_specs=[vmem] * 3,
        scratch_shapes=[
            pltpu.VMEM(incidence.shape, jnp.int32),
            pltpu.VMEM(phase.shape, jnp.bfloat16),
            pltpu.VMEM((1, triplets), jnp.float32),
            pltpu.VMEM((2, rows), jnp.int32),
            pltpu.VMEM((triplets, pixel_count), jnp.bfloat16),
            pltpu.VMEM((depth, pixel_count), jnp.bfloat16),
            pltpu.VMEM((8, 2 * LANES), jnp.bfloat16),
            pltpu.VMEM((LANES, LANES), jnp.float32),
            pltpu.VMEM((8, 2 * LANES), jnp.float32),
            pltpu.VMEM((depth, pixel_count), jnp.bfloat16),
            pltpu.VMEM((GROUP, depth, LANES), jnp.bfloat16),
            pltpu.VMEM((LANES, GROUP * depth), jnp.bfloat16),
            pltpu.VMEM((GROUP, 8, 2 * LANES), jnp.bfloat16),
            pltpu.VMEM((pairs, 8, 2 * LANES), jnp.float32),
            pltpu.VMEM((pairs, GROUP * depth, 2 * LANES), jnp.bfloat16),
            pltpu.VMEM((depth, 2 * LANES), jnp.bfloat16),
            pltpu.VMEM((2, LANES, 2 * LANES), jnp.float32),
            pltpu.VMEM((pairs, 2 * LANES, LANES), jnp.bfloat16),
            pltpu.VMEM((GROUP, depth, LANES), jnp.bfloat16),
            pltpu.VMEM((LANES, 2 * LANES), jnp.float32),
            pltpu.VMEM((pixes, 1, LANES), jnp.float32),
            pltpu.VMEM((2, LANES), jnp.float32),
            pltpu.VMEM((GROUP, 2, LANES), jnp.float32),
            pltpu.SemaphoreType.DMA((4,)),
            pltpu.SemaphoreType.DMA((2,)),
            pltpu.SemaphoreType.DMA((GROUP // 2,)),
            *[pltpu.SemaphoreType.DMA] * 11,
            *[pltpu.SemaphoreType.REGULAR] * 3,
        ],
        compiler_params=pltpu.CompilerParams(collective_id=0, has_side_effects=True, vmem_limit_bytes=VMEM),
    )(*operands)
    return pl.pallas_call(
        store,
        out_shape=(
            jax.ShapeDtypeStruct(residual.shape, jnp.float32),
            jax.ShapeDtypeStruct((pixel_count,), jnp.float32),
            jax.ShapeDtypeStruct(corrected.shape, jnp.float32),
        ),
        in_specs=[pl.BlockSpec(memory_space=pl.ANY)] * 3,
        out_specs=[hbm] * 3,
        scratch_shapes=[pltpu.SemaphoreType.DMA((6,))],
        compiler_params=pltpu.CompilerParams(vmem_limit_bytes=1024 * 1024),
    )(residual, relative, corrected)


def solution(mesh):
    return jax.shard_map(
        local,
        mesh=mesh,
        in_specs=(P("ifg", "pix"), P("ifg", None), P("ifg"), P("ifg", None)),
        out_specs=(P("ifg", "pix"), P("pix"), P("ifg", "pix")),
        check_vma=False,
    )
```

```python
import functools

import jax
import jax.numpy as jnp
from jax import lax
from jax.experimental import pallas as pl
from jax.experimental.pallas import tpu as pltpu
from jax.sharding import PartitionSpec as P

GROUP = 16
LANES = 128
EARLY = 2
VMEM = 16 * 1024 * 1024
INV_2PI = 0.15915494309189535
TWO_PI_HI = 6.28125
TWO_PI_LO = 1.9353071795864769e-3
SIN = (-0.041666642741103474, 0.000520813580633296, -3.094783609930149e-06, 1.0156463124188801e-08)
COS = (-0.12499999887388552, 0.0026041650454957602, -2.170063047895746e-05, 9.672611781418933e-08, -2.5465921654786513e-10)


def poly(coefs, z):
    out = z * coefs[-1] + coefs[-2]
    for c in coefs[-3::-1]:
        out = out * z + c
    return out


def sin_and_twice_loss(x):
    k = jnp.round(x * INV_2PI)
    r = (x - k * TWO_PI_HI) - k * TWO_PI_LO
    z = r * r
    sine = r + (r * z) * poly(SIN, z)
    cosine = 1.0 + z * poly(COS, z)
    return sine * cosine, sine * sine


PEERS = sorted(
    ((dx, dy) for dx in range(4) for dy in range(4) if dx or dy),
    key=lambda p: -min(p[0], 4 - p[0]) - min(p[1], 4 - p[1]),
)


def rank_of(device, core):
    x, y = device // 4, lax.rem(device, 4)
    return lax.rem(jnp.where(core == 0, y + x, y - x + 7), 4)


def kernel(
    all_pixels,
    phase_hbm, inc_hbm, weight_hbm, dates_hbm, residual_ref, rel_ref, corrected_ref,
    inc, phase, weight, dates, res_ref, cor_ref, idx, rest16, wrow, padded, ph, pht, idxs, tiles, inct, iota, clo, wb, cb, acc, scores, fin_out, fin,
    in_sem, ph_r, idx_r, idx_s, ph_s, res_s, res_r, lef_s, cor_s, cor_r, fin_s, fin_r, pix_s, pix_r,
    near1, near2, near4,
):
    me = lax.axis_index("ifg")
    pix = lax.axis_index("pix")
    x, y = me // 4, lax.rem(me, 4)
    core = lax.rem(pix, 2)
    rank = rank_of(me, core)
    active = rank < 3
    share = 3 * x + rank
    my_lanes = pl.ds(pl.multiple_of(share * LANES, LANES), LANES)
    rows = phase.shape[0]
    depth = padded.shape[0]
    pixes = scores.shape[0]
    steps = GROUP // 2 + 1

    def peer(dx, dy):
        return xs[dx] + ys[dy]

    xs = [4 * lax.rem(x + i, 4) for i in range(4)]
    ys = [lax.rem(y + i, 4) for i in range(4)]

    def far(k):
        return lax.rem(pix + pixes // 2 + (k + 1) // 2 * (1 - 2 * (k % 2)), pixes)

    barrier = pltpu.get_barrier_semaphore()

    def tell_pix(sem, other):
        pl.semaphore_signal(sem, inc=1, device_id={"pix": lax.rem(other, pixes)}, device_id_type=pl.DeviceIdType.MESH)

    def tell_along_z(sem, distance):
        tell_pix(sem, pix + 2 * distance)
        tell_pix(sem, pix + pixes - 2 * distance)

    for dx, dy in PEERS:
        pl.semaphore_signal(barrier, inc=1, device_id={"ifg": peer(dx, dy)}, device_id_type=pl.DeviceIdType.MESH)
    across = 2 * (pix // 2) + 1 - core
    tell_pix(barrier, across)
    tell_along_z(barrier, 1)
    tell_pix(barrier, across + 2)
    tell_pix(barrier, across + pixes - 2)
    read_inc = pltpu.make_async_copy(inc_hbm, inc, in_sem.at[0])
    read_inc.start()
    read_phase = pltpu.make_async_copy(phase_hbm, phase, in_sem.at[1])
    read_phase.start()
    read_weight = pltpu.make_async_copy(weight_hbm, weight, in_sem.at[2])
    read_weight.start()
    read_dates = pltpu.make_async_copy(dates_hbm, dates, in_sem.at[3])
    read_dates.start()

    iota[...] = lax.broadcasted_iota(jnp.int32, iota.shape, 0).astype(jnp.float32).astype(jnp.bfloat16)
    acc[...] = jnp.zeros_like(acc)
    scores[pix] = jnp.zeros(scores.shape[1:], scores.dtype)
    wrow[...] = jnp.zeros_like(wrow)
    rest16[...] = jnp.zeros_like(rest16)
    padded[...] = jnp.zeros_like(padded)

    read_inc.wait()
    read_phase.wait()
    read_weight.wait()
    read_dates.wait()
    padded[0:rows, :] = phase[...]
    wrow[0:1, 0 : weight.shape[1]] = weight[...]
    width = inc.shape[1]
    column = lax.broadcasted_iota(jnp.int32, (1, width), 1).astype(jnp.float32)
    value = inc[...]
    plus = value == 1
    first = jnp.min(jnp.where(plus, column, 4096.0), axis=1, keepdims=True)
    second = jnp.max(jnp.where(plus, column, -1.0), axis=1, keepdims=True)
    long = jnp.sum(jnp.where(value == -1, column, 0.0), axis=1, keepdims=True)
    lane = lax.broadcasted_iota(jnp.int32, (inc.shape[0], LANES), 1)
    three = jnp.where(lane == 0, first, jnp.where(lane == 1, second, long))
    spot = 16 * lax.rem(me, 8)
    rest16[pl.ds(pl.multiple_of(spot, 16), 16), :] = three[LANES:]
    here = lax.broadcasted_iota(jnp.int32, (8, LANES), 1) // 16 == lax.rem(me, 8)
    for q, t, w in (
        (0, three[:LANES], wrow[:, :LANES]),
        (1, rest16[...], pltpu.roll(wrow[:, LANES:], spot, 1)),
    ):
        t = jnp.transpose(t)[0:8]
        block = jnp.floor((t + 0.5) * (1.0 / rows))
        high = w[0:1].astype(jnp.bfloat16).astype(jnp.float32)
        message = jnp.concatenate([(t - block * rows)[0:3], block[0:3], high, w[0:1] - high], axis=0)
        idx[:, q * LANES : (q + 1) * LANES] = jnp.where(jnp.logical_or(q == 0, here), message, 0.0).astype(jnp.bfloat16)

    pl.semaphore_wait(barrier, GROUP + 4)
    tell_along_z(near1, 1)

    def put(src, dst, send, recv, device):
        pltpu.make_async_remote_copy(
            src_ref=src, dst_ref=dst, send_sem=send, recv_sem=recv,
            device_id={"ifg": device}, device_id_type=pl.DeviceIdType.MESH,
        ).start()

    def keep(src, dst, recv):
        pltpu.make_async_copy(src, dst, recv).start()

    def took(ref, sem):
        pltpu.make_async_copy(ref, ref, sem).wait()

    def to_shares(body, own):
        for c, e in ((c, e) for c in range(2) for e in (0, 1, 3, 2)):
            their = lax.rem(rank + e, 4)

            @pl.when(jnp.logical_and(core == c, their < 3))
            def _():
                for dx, dy in PEERS:
                    if (dy + dx * (1 - 2 * c)) % 4 == e:
                        at = pl.multiple_of((3 * lax.rem(x + dx, 4) + their) * LANES, LANES)
                        body(peer(dx, dy), at)
                if e == 0:
                    own()

    here_idx = idx_r.at[me // 2]
    here_ph = ph_r.at[me // 8]
    to_shares(lambda d, at: put(idx, idxs.at[me], idx_s, here_idx, d), lambda: keep(idx, idxs.at[me], here_idx))
    pl.semaphore_wait(near1, 2)
    tell_along_z(near2, 2)
    to_shares(
        lambda d, at: put(padded.at[:, pl.ds(at, LANES)], ph.at[me], ph_s, here_ph, d),
        lambda: keep(padded.at[:, my_lanes], ph.at[me], here_ph),
    )

    def pair(j):
        return lax.rem(me // 2 + 1 + j, GROUP // 2)

    def build(j):
        t = tiles[j]
        at = iota[...]
        lines = []
        blocks = []
        for i in range(3):
            row = jnp.broadcast_to(t[i : i + 1], at.shape).astype(jnp.bfloat16)
            lines.append(jnp.where(at == row, jnp.full_like(at, -1.0 if i == 2 else 1.0), jnp.zeros_like(at)))
            blocks.append(jnp.broadcast_to(t[3 + i : 4 + i], (16, at.shape[1])).astype(jnp.bfloat16))
        one = jnp.ones_like(blocks[0])
        for b in range(GROUP):
            inside = [jnp.where(v == one * b, one, jnp.zeros_like(one)) for v in blocks]
            for g in range(depth // 16):
                terms = [v * line[16 * g : 16 * g + 16] for v, line in zip(inside, lines)]
                inct[j, b * depth + 16 * g : b * depth + 16 * g + 16, :] = terms[0] + terms[1] + terms[2]

    def weights(j):
        return tiles[j, 6:7, :] + tiles[j, 7:8, :]

    def finish(j, count):
        lost = acc[...]
        for q in range(count):
            sine, loss = sin_and_twice_loss(clo[q])
            lost = lost + loss * (0.5 * weights(j + q))
            wb[j + q] = jnp.transpose(sine).astype(jnp.bfloat16)
        acc[...] = lost

    mine = res_ref.at[pl.ds(0, LANES), my_lanes]
    mine16 = res_ref.at[pl.ds(LANES, 16), my_lanes]

    def send_pair(j):
        for q in range(2):
            put(wb.at[j, pl.ds(q * LANES, LANES)], mine, res_s, res_r, 2 * pair(j) + q)

    def send_own_pair(j):
        odd = lax.rem(me, 2)
        own = pl.ds(pl.multiple_of(odd * LANES, LANES), LANES)
        next_door = pl.ds(pl.multiple_of((1 - odd) * LANES, LANES), LANES)
        put(wb.at[j, next_door], mine, res_s, res_r, me + 1 - 2 * odd)
        keep(wb.at[j, own], mine, res_r)

    @pl.when(rank == 3)
    def _():
        pl.semaphore_wait(near2, 2)
        tell_along_z(near4, 4)

    @pl.when(active)
    def _():
        def arrived(k):
            p = lax.rem(k + 1, GROUP // 2)
            j = lax.rem(p - me // 2 + GROUP // 2 - 1, GROUP // 2)
            took(idxs.at[pl.ds(2 * p, 2)], idx_r.at[p])
            for q in range(2):
                tiles[j, :, q * LANES : (q + 1) * LANES] = idxs[2 * p + q, :, 0:LANES].astype(jnp.float32)
            build(j)

        pl.loop(0, EARLY)(arrived)
        pl.semaphore_wait(near2, 2)
        tell_along_z(near4, 4)
        pl.loop(EARLY, GROUP // 2)(arrived)

        for q in range(2):
            rest = idxs[8 * q, :, LANES:].astype(jnp.float32)
            for i in range(1, 8):
                rest = rest + idxs[8 * q + i, :, LANES:].astype(jnp.float32)
            tiles[GROUP // 2, :, q * LANES : (q + 1) * LANES] = rest

        build(steps - 1)

        for half in range(2):
            took(ph.at[pl.ds(8 * half, 8)], ph_r.at[half])
            block = ph[8 * half : 8 * half + 8].reshape(8 * depth, LANES)
            pht[:, 8 * depth * half : 8 * depth * (half + 1)] = jnp.transpose(block.astype(jnp.float32)).astype(jnp.bfloat16)

        def multiply(j):
            return jnp.dot(pht[...], inct[j], preferred_element_type=jnp.float32)

        for q in range(2):
            clo[q] = multiply(q)

        @pl.loop(1, GROUP // 4)
        def _(g):
            closure = [multiply(2 * g + q) for q in range(2)]
            finish(2 * g - 2, 2)
            for q in range(2):
                clo[q] = closure[q]
            for q in range(2):
                send_pair(2 * g - 2 + q)

        closure = multiply(steps - 1)
        finish(steps - 3, 2)
        clo[0] = closure
        finish(steps - 1, 1)

        total = weights(0)
        for j in range(1, steps):
            total = total + weights(j)
        both = acc[:, 0:LANES] + acc[:, LANES:]
        misfit = jnp.sum(jnp.transpose(both), axis=0, keepdims=True)
        scores[pix] = misfit / jnp.sum(total, axis=1, keepdims=True)

    pl.semaphore_wait(near4, 2)

    for k in range(pixes - 1):
        pltpu.make_async_remote_copy(
            src_ref=scores.at[pix], dst_ref=scores.at[pix], send_sem=pix_s, recv_sem=pix_r,
            device_id={"pix": far(k)}, device_id_type=pl.DeviceIdType.MESH,
        ).start()

    @pl.when(active)
    def _():
        send_pair(steps - 3)
        send_own_pair(steps - 2)

        def sixteen(d):
            return wb.at[steps - 1, pl.ds(pl.multiple_of(16 * d, 16), 16)]

        for dx, dy in PEERS:
            put(sixteen(peer(dx, dy)), mine16, lef_s, res_r, peer(dx, dy))
        keep(sixteen(me), mine16, res_r)

        @pl.loop(0, 4)
        def _(j):
            c = lax.rem(x + 2 + j, 4)
            at = pl.ds(pl.multiple_of(c * 4 * depth, 4 * depth), 4 * depth)
            corr = jnp.zeros((4 * depth, LANES), jnp.float32)
            for p in range(steps):
                corr = corr + jnp.dot(inct[p, at, :], wb[p], preferred_element_type=jnp.float32)
            cb[pl.ds(4 * c, 4)] = corr.astype(jnp.bfloat16).reshape(4, depth, LANES)
            for q in range(4):
                d = 4 * c + q

                @pl.when(d != me)
                def _():
                    put(cb.at[d], cor_ref.at[:, my_lanes], cor_s, cor_r, d)

                @pl.when(d == me)
                def _():
                    keep(cb.at[d], cor_ref.at[:, my_lanes], cor_r)

    took(scores.at[pl.ds(0, pixes - 1)], pix_r)

    fin_out[0:1] = scores[pix]
    fin_out[1:2] = jnp.sum(scores[...], axis=0)
    slot = jnp.where(active, share, 12 + x)

    for dx, dy in PEERS:
        put(fin_out, fin.at[slot], fin_s, fin_r, peer(dx, dy))
    keep(fin_out, fin.at[slot], fin_r)

    others = GROUP - 1
    took(scores.at[pl.ds(0, pixes - 1)], pix_s)

    @pl.when(active)
    def _():
        took(idxs.at[pl.ds(0, 11)], idx_s)
        took(ph.at[pl.ds(0, 11)], ph_s)
        took(inct.at[0, pl.ds(0, others * LANES // 2)], res_s)
        took(wb.at[0, pl.ds(0, others * 16)], lef_s)
        took(cb.at[pl.ds(0, others)], cor_s)

    @pl.when(rank == 3)
    def _():
        took(idxs.at[pl.ds(0, 12)], idx_s)
        took(ph.at[pl.ds(0, 12)], ph_s)

    took(res_ref, res_r)
    took(cor_ref, cor_r)

    span = (dates[1:2] - dates[0:1]).astype(jnp.float32)
    damp = jnp.concatenate([1.0 / (2.0 + span), jnp.zeros((1, LANES - rows), jnp.float32)], axis=1)
    damp = jnp.transpose(jnp.broadcast_to(damp, (LANES, LANES)))[:rows]

    @pl.loop(0, 12)
    def _(s):
        lanes = pl.ds(pl.multiple_of(s * LANES, LANES), LANES)
        residual_ref[:, lanes] = res_ref[:, lanes].astype(jnp.float32)
        corrected_ref[:, lanes] = phase[:, lanes].astype(jnp.float32) - cor_ref[0:rows, lanes].astype(jnp.float32) * damp

    took(fin.at[pl.ds(0, others)], fin_s)
    took(fin, fin_r)

    everything = jnp.sum(jnp.sum(fin[...], axis=0)[1:2], axis=1, keepdims=True)
    for s in range(12):
        rel_ref[:, s * LANES : (s + 1) * LANES] = fin[s, 0:1] / (everything / all_pixels)


def store(residual, relative, corrected, residual_out, relative_out, corrected_out, sems):
    copies = [(relative.at[0], relative_out)]
    for src, dst, step in ((residual, residual_out, 48), (corrected, corrected_out, 40)):
        for at in range(0, src.shape[0], step):
            rows = pl.ds(at, min(step, src.shape[0] - at))
            copies.append((src.at[rows], dst.at[rows]))
    copies = [pltpu.make_async_copy(src, dst, sems.at[i]) for i, (src, dst) in enumerate(copies)]
    for copy in copies:
        copy.start()
    for copy in copies:
        copy.wait()


def local(phase, incidence, triplet_weight, date_pairs):
    rows, pixel_count = phase.shape
    depth = -(-rows // 16) * 16
    triplets = incidence.shape[0]
    pairs = GROUP // 2 + 1
    hbm = pl.BlockSpec(memory_space=pltpu.HBM)
    vmem = pl.BlockSpec(memory_space=pltpu.VMEM)
    pixes = lax.axis_size("pix")
    operands = (phase, incidence, triplet_weight.reshape(1, triplets), date_pairs.T)
    operands = [pltpu.with_memory_space_constraint(a, pltpu.HBM) for a in operands]
    residual, relative, corrected = pl.pallas_call(
        functools.partial(kernel, pixes * pixel_count),
        out_shape=(
            jax.ShapeDtypeStruct((triplets, pixel_count), jnp.float32),
            jax.ShapeDtypeStruct((1, pixel_count), jnp.float32),
            jax.ShapeDtypeStruct((rows, pixel_count), jnp.float32),
        ),
        in_specs=[hbm] * 4,
        out_specs=[vmem] * 3,
        scratch_shapes=[
            pltpu.VMEM(incidence.shape, jnp.int32),
            pltpu.VMEM(phase.shape, jnp.bfloat16),
            pltpu.VMEM((1, triplets), jnp.float32),
            pltpu.VMEM((2, rows), jnp.int32),
            pltpu.VMEM((triplets, pixel_count), jnp.bfloat16),
            pltpu.VMEM((depth, pixel_count), jnp.bfloat16),
            pltpu.VMEM((8, 2 * LANES), jnp.bfloat16),
            pltpu.VMEM((LANES, LANES), jnp.float32),
            pltpu.VMEM((8, 2 * LANES), jnp.float32),
            pltpu.VMEM((depth, pixel_count), jnp.bfloat16),
            pltpu.VMEM((GROUP, depth, LANES), jnp.bfloat16),
            pltpu.VMEM((LANES, GROUP * depth), jnp.bfloat16),
            pltpu.VMEM((GROUP, 8, 2 * LANES), jnp.bfloat16),
            pltpu.VMEM((pairs, 8, 2 * LANES), jnp.float32),
            pltpu.VMEM((pairs, GROUP * depth, 2 * LANES), jnp.bfloat16),
            pltpu.VMEM((depth, 2 * LANES), jnp.bfloat16),
            pltpu.VMEM((2, LANES, 2 * LANES), jnp.float32),
            pltpu.VMEM((pairs, 2 * LANES, LANES), jnp.bfloat16),
            pltpu.VMEM((GROUP, depth, LANES), jnp.bfloat16),
            pltpu.VMEM((LANES, 2 * LANES), jnp.float32),
            pltpu.VMEM((pixes, 1, LANES), jnp.float32),
            pltpu.VMEM((2, LANES), jnp.float32),
            pltpu.VMEM((GROUP, 2, LANES), jnp.float32),
            pltpu.SemaphoreType.DMA((4,)),
            pltpu.SemaphoreType.DMA((2,)),
            pltpu.SemaphoreType.DMA((GROUP // 2,)),
            *[pltpu.SemaphoreType.DMA] * 11,
            *[pltpu.SemaphoreType.REGULAR] * 3,
        ],
        compiler_params=pltpu.CompilerParams(collective_id=0, has_side_effects=True, vmem_limit_bytes=VMEM),
    )(*operands)
    return pl.pallas_call(
        store,
        out_shape=(
            jax.ShapeDtypeStruct(residual.shape, jnp.float32),
            jax.ShapeDtypeStruct((pixel_count,), jnp.float32),
            jax.ShapeDtypeStruct(corrected.shape, jnp.float32),
        ),
        in_specs=[pl.BlockSpec(memory_space=pl.ANY)] * 3,
        out_specs=[hbm] * 3,
        scratch_shapes=[pltpu.SemaphoreType.DMA((6,))],
        compiler_params=pltpu.CompilerParams(vmem_limit_bytes=1024 * 1024),
    )(residual, relative, corrected)


def solution(mesh):
    return jax.shard_map(
        local,
        mesh=mesh,
        in_specs=(P("ifg", "pix"), P("ifg", None), P("ifg"), P("ifg", None)),
        out_specs=(P("ifg", "pix"), P("pix"), P("ifg", "pix")),
        check_vma=False,
    )
```

```python
import functools

import jax
import jax.numpy as jnp
from jax import lax
from jax.experimental import pallas as pl
from jax.experimental.pallas import tpu as pltpu
from jax.sharding import PartitionSpec as P

GROUP = 16
LANES = 128
EARLY = 2
VMEM = 16 * 1024 * 1024
INV_2PI = 0.15915494309189535
TWO_PI_HI = 6.28125
TWO_PI_LO = 1.9353071795864769e-3
SIN = (-0.041666642741103474, 0.000520813580633296, -3.094783609930149e-06, 1.0156463124188801e-08)
COS = (-0.12499999887388552, 0.0026041650454957602, -2.170063047895746e-05, 9.672611781418933e-08, -2.5465921654786513e-10)


def poly(coefs, z):
    out = z * coefs[-1] + coefs[-2]
    for c in coefs[-3::-1]:
        out = out * z + c
    return out


def sin_and_twice_loss(x):
    k = jnp.round(x * INV_2PI)
    r = (x - k * TWO_PI_HI) - k * TWO_PI_LO
    z = r * r
    sine = r + (r * z) * poly(SIN, z)
    cosine = 1.0 + z * poly(COS, z)
    return sine * cosine, sine * sine


PEERS = sorted(
    ((dx, dy) for dx in range(4) for dy in range(4) if dx or dy),
    key=lambda p: -min(p[0], 4 - p[0]) - min(p[1], 4 - p[1]),
)


def rank_of(device, core):
    x, y = device // 4, lax.rem(device, 4)
    return lax.rem(jnp.where(core == 0, y + x, y - x + 7), 4)


def kernel(
    all_pixels,
    phase_hbm, inc_hbm, weight_hbm, dates_hbm, residual_ref, rel_ref, corrected_ref,
    inc, phase, weight, dates, res_ref, cor_ref, idx, rest16, wrow, padded, ph, pht, idxs, tiles, inct, iota, clo, wb, cb, acc, scores, fin_out, fin,
    in_sem, ph_r, idx_r, idx_s, ph_s, res_s, res_r, lef_s, cor_s, cor_r, fin_s, fin_r, pix_s, pix_r,
    near1, near2, near4,
):
    me = lax.axis_index("ifg")
    pix = lax.axis_index("pix")
    x, y = me // 4, lax.rem(me, 4)
    core = lax.rem(pix, 2)
    rank = rank_of(me, core)
    active = rank < 3
    share = 3 * x + rank
    my_lanes = pl.ds(pl.multiple_of(share * LANES, LANES), LANES)
    rows = phase.shape[0]
    depth = padded.shape[0]
    pixes = scores.shape[0]
    steps = GROUP // 2 + 1

    def peer(dx, dy):
        return xs[dx] + ys[dy]

    xs = [4 * lax.rem(x + i, 4) for i in range(4)]
    ys = [lax.rem(y + i, 4) for i in range(4)]

    def far(k):
        return lax.rem(pix + pixes // 2 + (k + 1) // 2 * (1 - 2 * (k % 2)), pixes)

    barrier = pltpu.get_barrier_semaphore()

    def tell_pix(sem, other):
        pl.semaphore_signal(sem, inc=1, device_id={"pix": lax.rem(other, pixes)}, device_id_type=pl.DeviceIdType.MESH)

    def tell_along_z(sem, distance):
        tell_pix(sem, pix + 2 * distance)
        tell_pix(sem, pix + pixes - 2 * distance)

    read_inc = pltpu.make_async_copy(inc_hbm, inc, in_sem.at[0])
    read_inc.start()
    for dx, dy in PEERS:
        pl.semaphore_signal(barrier, inc=1, device_id={"ifg": peer(dx, dy)}, device_id_type=pl.DeviceIdType.MESH)
    across = 2 * (pix // 2) + 1 - core
    tell_pix(barrier, across)
    tell_along_z(barrier, 1)
    tell_pix(barrier, across + 2)
    tell_pix(barrier, across + pixes - 2)
    read_phase = pltpu.make_async_copy(phase_hbm, phase, in_sem.at[1])
    read_phase.start()
    read_weight = pltpu.make_async_copy(weight_hbm, weight, in_sem.at[2])
    read_weight.start()
    read_dates = pltpu.make_async_copy(dates_hbm, dates, in_sem.at[3])
    read_dates.start()

    iota[...] = lax.broadcasted_iota(jnp.int32, iota.shape, 0).astype(jnp.float32).astype(jnp.bfloat16)
    acc[...] = jnp.zeros_like(acc)
    scores[pix] = jnp.zeros(scores.shape[1:], scores.dtype)
    wrow[...] = jnp.zeros_like(wrow)
    rest16[...] = jnp.zeros_like(rest16)
    padded[...] = jnp.zeros_like(padded)

    read_inc.wait()
    read_phase.wait()
    read_weight.wait()
    read_dates.wait()
    padded[0:rows, :] = phase[...]
    wrow[0:1, 0 : weight.shape[1]] = weight[...]
    width = inc.shape[1]
    column = lax.broadcasted_iota(jnp.int32, (1, width), 1).astype(jnp.float32)
    value = inc[...]
    plus = value == 1
    first = jnp.min(jnp.where(plus, column, 4096.0), axis=1, keepdims=True)
    second = jnp.max(jnp.where(plus, column, -1.0), axis=1, keepdims=True)
    long = jnp.sum(jnp.where(value == -1, column, 0.0), axis=1, keepdims=True)
    lane = lax.broadcasted_iota(jnp.int32, (inc.shape[0], LANES), 1)
    three = jnp.where(lane == 0, first, jnp.where(lane == 1, second, long))
    spot = 16 * lax.rem(me, 8)
    rest16[pl.ds(pl.multiple_of(spot, 16), 16), :] = three[LANES:]
    here = lax.broadcasted_iota(jnp.int32, (8, LANES), 1) // 16 == lax.rem(me, 8)
    for q, t, w in (
        (0, three[:LANES], wrow[:, :LANES]),
        (1, rest16[...], pltpu.roll(wrow[:, LANES:], spot, 1)),
    ):
        t = jnp.transpose(t)[0:8]
        block = jnp.floor((t + 0.5) * (1.0 / rows))
        high = w[0:1].astype(jnp.bfloat16).astype(jnp.float32)
        message = jnp.concatenate([(t - block * rows)[0:3], block[0:3], high, w[0:1] - high], axis=0)
        idx[:, q * LANES : (q + 1) * LANES] = jnp.where(jnp.logical_or(q == 0, here), message, 0.0).astype(jnp.bfloat16)

    pl.semaphore_wait(barrier, GROUP + 4)
    tell_along_z(near1, 1)

    def put(src, dst, send, recv, device):
        pltpu.make_async_remote_copy(
            src_ref=src, dst_ref=dst, send_sem=send, recv_sem=recv,
            device_id={"ifg": device}, device_id_type=pl.DeviceIdType.MESH,
        ).start()

    def keep(src, dst, recv):
        pltpu.make_async_copy(src, dst, recv).start()

    def took(ref, sem):
        pltpu.make_async_copy(ref, ref, sem).wait()

    def to_shares(body, own):
        for c, e in ((c, e) for c in range(2) for e in (0, 1, 3, 2)):
            their = lax.rem(rank + e, 4)

            @pl.when(jnp.logical_and(core == c, their < 3))
            def _():
                for dx, dy in PEERS:
                    if (dy + dx * (1 - 2 * c)) % 4 == e:
                        at = pl.multiple_of((3 * lax.rem(x + dx, 4) + their) * LANES, LANES)
                        body(peer(dx, dy), at)
                if e == 0:
                    own()

    here_idx = idx_r.at[me // 2]
    here_ph = ph_r.at[me // 8]
    to_shares(lambda d, at: put(idx, idxs.at[me], idx_s, here_idx, d), lambda: keep(idx, idxs.at[me], here_idx))
    pl.semaphore_wait(near1, 2)
    tell_along_z(near2, 2)
    to_shares(
        lambda d, at: put(padded.at[:, pl.ds(at, LANES)], ph.at[me], ph_s, here_ph, d),
        lambda: keep(padded.at[:, my_lanes], ph.at[me], here_ph),
    )

    def pair(j):
        return lax.rem(me // 2 + 1 + j, GROUP // 2)

    def build(j):
        t = tiles[j]
        at = iota[...]
        lines = []
        blocks = []
        for i in range(3):
            row = jnp.broadcast_to(t[i : i + 1], at.shape).astype(jnp.bfloat16)
            lines.append(jnp.where(at == row, jnp.full_like(at, -1.0 if i == 2 else 1.0), jnp.zeros_like(at)))
            blocks.append(jnp.broadcast_to(t[3 + i : 4 + i], (16, at.shape[1])).astype(jnp.bfloat16))
        one = jnp.ones_like(blocks[0])
        for b in range(GROUP):
            inside = [jnp.where(v == one * b, one, jnp.zeros_like(one)) for v in blocks]
            for g in range(depth // 16):
                terms = [v * line[16 * g : 16 * g + 16] for v, line in zip(inside, lines)]
                inct[j, b * depth + 16 * g : b * depth + 16 * g + 16, :] = terms[0] + terms[1] + terms[2]

    def weights(j):
        return tiles[j, 6:7, :] + tiles[j, 7:8, :]

    def finish(j, count):
        lost = acc[...]
        for q in range(count):
            sine, loss = sin_and_twice_loss(clo[q])
            lost = lost + loss * (0.5 * weights(j + q))
            wb[j + q] = jnp.transpose(sine).astype(jnp.bfloat16)
        acc[...] = lost

    mine = res_ref.at[pl.ds(0, LANES), my_lanes]
    mine16 = res_ref.at[pl.ds(LANES, 16), my_lanes]

    def send_pair(j):
        for q in range(2):
            put(wb.at[j, pl.ds(q * LANES, LANES)], mine, res_s, res_r, 2 * pair(j) + q)

    def send_own_pair(j):
        odd = lax.rem(me, 2)
        own = pl.ds(pl.multiple_of(odd * LANES, LANES), LANES)
        next_door = pl.ds(pl.multiple_of((1 - odd) * LANES, LANES), LANES)
        put(wb.at[j, next_door], mine, res_s, res_r, me + 1 - 2 * odd)
        keep(wb.at[j, own], mine, res_r)

    @pl.when(rank == 3)
    def _():
        pl.semaphore_wait(near2, 2)
        tell_along_z(near4, 4)

    @pl.when(active)
    def _():
        def arrived(k):
            p = lax.rem(k + 1, GROUP // 2)
            j = lax.rem(p - me // 2 + GROUP // 2 - 1, GROUP // 2)
            took(idxs.at[pl.ds(2 * p, 2)], idx_r.at[p])
            for q in range(2):
                tiles[j, :, q * LANES : (q + 1) * LANES] = idxs[2 * p + q, :, 0:LANES].astype(jnp.float32)
            build(j)

        pl.loop(0, EARLY)(arrived)
        pl.semaphore_wait(near2, 2)
        tell_along_z(near4, 4)
        pl.loop(EARLY, GROUP // 2)(arrived)

        for q in range(2):
            rest = idxs[8 * q, :, LANES:].astype(jnp.float32)
            for i in range(1, 8):
                rest = rest + idxs[8 * q + i, :, LANES:].astype(jnp.float32)
            tiles[GROUP // 2, :, q * LANES : (q + 1) * LANES] = rest

        build(steps - 1)

        for half in range(2):
            took(ph.at[pl.ds(8 * half, 8)], ph_r.at[half])
            block = ph[8 * half : 8 * half + 8].reshape(8 * depth, LANES)
            pht[:, 8 * depth * half : 8 * depth * (half + 1)] = jnp.transpose(block.astype(jnp.float32)).astype(jnp.bfloat16)

        def multiply(j):
            return jnp.dot(pht[...], inct[j], preferred_element_type=jnp.float32)

        for q in range(2):
            clo[q] = multiply(q)

        @pl.loop(1, GROUP // 4)
        def _(g):
            closure = [multiply(2 * g + q) for q in range(2)]
            finish(2 * g - 2, 2)
            for q in range(2):
                clo[q] = closure[q]
            for q in range(2):
                send_pair(2 * g - 2 + q)

        closure = multiply(steps - 1)
        finish(steps - 3, 2)
        clo[0] = closure
        finish(steps - 1, 1)

        total = weights(0)
        for j in range(1, steps):
            total = total + weights(j)
        both = acc[:, 0:LANES] + acc[:, LANES:]
        misfit = jnp.sum(jnp.transpose(both), axis=0, keepdims=True)
        scores[pix] = misfit / jnp.sum(total, axis=1, keepdims=True)

    pl.semaphore_wait(near4, 2)

    for k in range(pixes - 1):
        pltpu.make_async_remote_copy(
            src_ref=scores.at[pix], dst_ref=scores.at[pix], send_sem=pix_s, recv_sem=pix_r,
            device_id={"pix": far(k)}, device_id_type=pl.DeviceIdType.MESH,
        ).start()

    @pl.when(active)
    def _():
        send_pair(steps - 3)
        send_own_pair(steps - 2)

        def sixteen(d):
            return wb.at[steps - 1, pl.ds(pl.multiple_of(16 * d, 16), 16)]

        for dx, dy in PEERS:
            put(sixteen(peer(dx, dy)), mine16, lef_s, res_r, peer(dx, dy))
        keep(sixteen(me), mine16, res_r)

        @pl.loop(0, 4)
        def _(j):
            c = lax.rem(x + 2 + j, 4)
            at = pl.ds(pl.multiple_of(c * 4 * depth, 4 * depth), 4 * depth)
            corr = jnp.zeros((4 * depth, LANES), jnp.float32)
            for p in range(steps):
                corr = corr + jnp.dot(inct[p, at, :], wb[p], preferred_element_type=jnp.float32)
            cb[pl.ds(4 * c, 4)] = corr.astype(jnp.bfloat16).reshape(4, depth, LANES)
            for q in range(4):
                d = 4 * c + q

                @pl.when(d != me)
                def _():
                    put(cb.at[d], cor_ref.at[:, my_lanes], cor_s, cor_r, d)

                @pl.when(d == me)
                def _():
                    keep(cb.at[d], cor_ref.at[:, my_lanes], cor_r)

    took(scores.at[pl.ds(0, pixes - 1)], pix_r)

    fin_out[0:1] = scores[pix]
    fin_out[1:2] = jnp.sum(scores[...], axis=0)
    slot = jnp.where(active, share, 12 + x)

    for dx, dy in PEERS:
        put(fin_out, fin.at[slot], fin_s, fin_r, peer(dx, dy))
    keep(fin_out, fin.at[slot], fin_r)

    others = GROUP - 1
    took(scores.at[pl.ds(0, pixes - 1)], pix_s)

    @pl.when(active)
    def _():
        took(idxs.at[pl.ds(0, 11)], idx_s)
        took(ph.at[pl.ds(0, 11)], ph_s)
        took(inct.at[0, pl.ds(0, others * LANES // 2)], res_s)
        took(wb.at[0, pl.ds(0, others * 16)], lef_s)
        took(cb.at[pl.ds(0, others)], cor_s)

    @pl.when(rank == 3)
    def _():
        took(idxs.at[pl.ds(0, 12)], idx_s)
        took(ph.at[pl.ds(0, 12)], ph_s)

    took(res_ref, res_r)
    took(cor_ref, cor_r)

    span = (dates[1:2] - dates[0:1]).astype(jnp.float32)
    damp = jnp.concatenate([1.0 / (2.0 + span), jnp.zeros((1, LANES - rows), jnp.float32)], axis=1)
    damp = jnp.transpose(jnp.broadcast_to(damp, (LANES, LANES)))[:rows]

    @pl.loop(0, 12)
    def _(s):
        lanes = pl.ds(pl.multiple_of(s * LANES, LANES), LANES)
        residual_ref[:, lanes] = res_ref[:, lanes].astype(jnp.float32)
        corrected_ref[:, lanes] = phase[:, lanes].astype(jnp.float32) - cor_ref[0:rows, lanes].astype(jnp.float32) * damp

    took(fin.at[pl.ds(0, others)], fin_s)
    took(fin, fin_r)

    everything = jnp.sum(jnp.sum(fin[...], axis=0)[1:2], axis=1, keepdims=True)
    for s in range(12):
        rel_ref[:, s * LANES : (s + 1) * LANES] = fin[s, 0:1] / (everything / all_pixels)


def store(residual, relative, corrected, residual_out, relative_out, corrected_out, sems):
    copies = [(relative.at[0], relative_out)]
    for src, dst, step in ((residual, residual_out, 144), (corrected, corrected_out, 80)):
        for at in range(0, src.shape[0], step):
            rows = pl.ds(at, min(step, src.shape[0] - at))
            copies.append((src.at[rows], dst.at[rows]))
    copies = [pltpu.make_async_copy(src, dst, sems.at[i]) for i, (src, dst) in enumerate(copies)]
    for copy in copies:
        copy.start()
    for copy in copies:
        copy.wait()


def local(phase, incidence, triplet_weight, date_pairs):
    rows, pixel_count = phase.shape
    depth = -(-rows // 16) * 16
    triplets = incidence.shape[0]
    pairs = GROUP // 2 + 1
    hbm = pl.BlockSpec(memory_space=pltpu.HBM)
    vmem = pl.BlockSpec(memory_space=pltpu.VMEM)
    pixes = lax.axis_size("pix")
    operands = (phase, incidence, triplet_weight.reshape(1, triplets), date_pairs.T)
    operands = [pltpu.with_memory_space_constraint(a, pltpu.HBM) for a in operands]
    residual, relative, corrected = pl.pallas_call(
        functools.partial(kernel, pixes * pixel_count),
        out_shape=(
            jax.ShapeDtypeStruct((triplets, pixel_count), jnp.float32),
            jax.ShapeDtypeStruct((1, pixel_count), jnp.float32),
            jax.ShapeDtypeStruct((rows, pixel_count), jnp.float32),
        ),
        in_specs=[hbm] * 4,
        out_specs=[vmem] * 3,
        scratch_shapes=[
            pltpu.VMEM(incidence.shape, jnp.int32),
            pltpu.VMEM(phase.shape, jnp.bfloat16),
            pltpu.VMEM((1, triplets), jnp.float32),
            pltpu.VMEM((2, rows), jnp.int32),
            pltpu.VMEM((triplets, pixel_count), jnp.bfloat16),
            pltpu.VMEM((depth, pixel_count), jnp.bfloat16),
            pltpu.VMEM((8, 2 * LANES), jnp.bfloat16),
            pltpu.VMEM((LANES, LANES), jnp.float32),
            pltpu.VMEM((8, 2 * LANES), jnp.float32),
            pltpu.VMEM((depth, pixel_count), jnp.bfloat16),
            pltpu.VMEM((GROUP, depth, LANES), jnp.bfloat16),
            pltpu.VMEM((LANES, GROUP * depth), jnp.bfloat16),
            pltpu.VMEM((GROUP, 8, 2 * LANES), jnp.bfloat16),
            pltpu.VMEM((pairs, 8, 2 * LANES), jnp.float32),
            pltpu.VMEM((pairs, GROUP * depth, 2 * LANES), jnp.bfloat16),
            pltpu.VMEM((depth, 2 * LANES), jnp.bfloat16),
            pltpu.VMEM((2, LANES, 2 * LANES), jnp.float32),
            pltpu.VMEM((pairs, 2 * LANES, LANES), jnp.bfloat16),
            pltpu.VMEM((GROUP, depth, LANES), jnp.bfloat16),
            pltpu.VMEM((LANES, 2 * LANES), jnp.float32),
            pltpu.VMEM((pixes, 1, LANES), jnp.float32),
            pltpu.VMEM((2, LANES), jnp.float32),
            pltpu.VMEM((GROUP, 2, LANES), jnp.float32),
            pltpu.SemaphoreType.DMA((4,)),
            pltpu.SemaphoreType.DMA((2,)),
            pltpu.SemaphoreType.DMA((GROUP // 2,)),
            *[pltpu.SemaphoreType.DMA] * 11,
            *[pltpu.SemaphoreType.REGULAR] * 3,
        ],
        compiler_params=pltpu.CompilerParams(collective_id=0, has_side_effects=True, vmem_limit_bytes=VMEM),
    )(*operands)
    return pl.pallas_call(
        store,
        out_shape=(
            jax.ShapeDtypeStruct(residual.shape, jnp.float32),
            jax.ShapeDtypeStruct((pixel_count,), jnp.float32),
            jax.ShapeDtypeStruct(corrected.shape, jnp.float32),
        ),
        in_specs=[pl.BlockSpec(memory_space=pl.ANY)] * 3,
        out_specs=[hbm] * 3,
        scratch_shapes=[pltpu.SemaphoreType.DMA((3,))],
        compiler_params=pltpu.CompilerParams(vmem_limit_bytes=1024 * 1024),
    )(residual, relative, corrected)


def solution(mesh):
    return jax.shard_map(
        local,
        mesh=mesh,
        in_specs=(P("ifg", "pix"), P("ifg", None), P("ifg"), P("ifg", None)),
        out_specs=(P("ifg", "pix"), P("pix"), P("ifg", "pix")),
        check_vma=False,
    )
```
